256 devices in a mesh: batch: 16 (over z_hi, y), ctx: 16 (over z_lo, x, core).
Axes of the slice: x: 4, y: 4, z: 8 (z_hi: 4, z_lo: 2; z = z_hi * 2 + z_lo), core: 2. Of those that a mesh axis runs over, the one named last changes fastest.
Arguments:
- asked_for: bfloat16 [32, 4096, 16, 128], P('batch', 'ctx'), may hold values from -6 to 6
- offered: bfloat16 [32, 4096, 16, 128], P('batch', 'ctx'), may hold values from -6 to 6
- contents: bfloat16 [32, 4096, 16, 128], P('batch', 'ctx'), may hold values from -6 to 6
- gate_rows: bfloat16 [32, 4096, 16, 128], P('batch', 'ctx'), may hold values from -6 to 6
- out_weight: bfloat16 [2048, 2048], P('batch'), may hold values from -0.125 to 0.125
Outputs:
- block_out: bfloat16 [32, 4096, 2048], P('batch', 'ctx')
The draws below stay inside these ranges and needn't reach their ends.
All inputs are finite; a program needn't handle non-finite values.
Results may differ from the reference program's by a relative error of at most 0.006.
Values may be sent and summed in bfloat16 or wider, within the bound.
A program may use at most 128 MiB of HBM per device.

```python
import jax
import jax.numpy as jnp
from jax import lax

HEADS = 16
HEAD_SIZE = 128
BATCH = 32
TOKENS = 4096
WIDTH = 2048


def shard_levels(key, shape, shards, low, high):
    def one(dim, parts):
        heights = jax.random.uniform(jax.random.fold_in(jax.random.fold_in(key, 6), dim), (parts,), jnp.float32, low / len(shards), high / len(shards))
        return jnp.repeat(jnp.exp(heights), shape[dim] // parts).reshape((-1,) + (1,) * (len(shape) - dim - 1))

    factor_of = one(*shards[0])
    for cut in shards[1:]:
        factor_of = factor_of * one(*cut)
    return factor_of


def normal_values(rng, extent, deviation, limit, split=(), dtype=jnp.bfloat16):
    values = deviation * jax.random.normal(rng, extent, jnp.float32)
    if split:
        values = values * shard_levels(rng, extent, split, -0.22, 0.18)
    return jnp.clip(values, -limit, limit).astype(dtype)


def setup_inputs(seed: int = 0) -> dict:
    key_of = jax.random.split(jax.random.key(seed), 6)
    asked_for = normal_values(key_of[0], (BATCH, TOKENS, HEADS, HEAD_SIZE), 1.0, 6.0, ((0, 16), (1, 16)))
    offered = normal_values(key_of[1], (BATCH, TOKENS, HEADS, HEAD_SIZE), 1.0, 6.0, ((0, 16), (1, 16)))
    contents = normal_values(key_of[2], (BATCH, TOKENS, HEADS, HEAD_SIZE), 1.0, 6.0, ((0, 16), (1, 16)))
    gate_rows = normal_values(key_of[3], (BATCH, TOKENS, HEADS, HEAD_SIZE), 1.0, 6.0, ((0, 16), (1, 16)))
    out_weight = normal_values(key_of[4], (WIDTH, WIDTH), WIDTH ** -0.5, 0.125, ((0, 16),))
    return {"asked_for": asked_for, "offered": offered, "contents": contents, "gate_rows": gate_rows, "out_weight": out_weight}


def to_features(values):
    wide = values.astype(jnp.float32)
    return (jnp.where(wide > 0.0, wide + 1.0, jnp.exp(jnp.minimum(wide, 0.0)))).astype(jnp.bfloat16)


def close_heads(read, gate_rows, count):
    result = read * count ** 0.5
    result = result * jax.nn.sigmoid(gate_rows.astype(jnp.float32))
    return result.astype(jnp.bfloat16)


def ask_state(features, state, mass):
    small = lax.optimization_barrier(state.astype(jnp.bfloat16))
    top = jnp.einsum("bthd,bhde->bthe", features.astype(jnp.float32), small.astype(jnp.float32))
    bottom = jnp.einsum("bthd,bhd->bth", features.astype(jnp.float32), mass, precision=lax.Precision.HIGHEST)
    return top / (bottom + 1e-3)[..., None]


def reference(asked_for, offered, contents, gate_rows, out_weight):
    query_feature, key_feature = lax.optimization_barrier((to_features(asked_for), to_features(offered)))
    state = jnp.einsum("bthd,bthe->bhde", key_feature.astype(jnp.float32), contents.astype(jnp.float32)) / TOKENS
    mass = jnp.sum(key_feature.astype(jnp.float32), axis=1) / TOKENS
    mixed = close_heads(ask_state(query_feature, state, mass), gate_rows, TOKENS).reshape(BATCH, TOKENS, WIDTH)
    mixed = lax.optimization_barrier(mixed)
    block_out = jnp.einsum("btw,wv->btv", mixed.astype(jnp.float32), out_weight.astype(jnp.float32)).astype(jnp.bfloat16)
    return block_out
```

```python
import jax
import jax.numpy as jnp
from jax import lax
from jax.experimental import pallas as pl
from jax.experimental.pallas import tpu as pltpu
from jax.sharding import Mesh
from jax.sharding import PartitionSpec as P

F32, BF16 = jnp.float32, jnp.bfloat16
MESH = pl.DeviceIdType.MESH
HEADS, SIZE = 16, 128
SEQS, ROWS = 2, 256
WIDTH = HEADS * SIZE
OFFSETS = (0, 3, 1, 2)


def feature(x):
    wide = x.astype(F32)
    return jnp.where(wide > 0.0, wide + 1.0, jnp.exp(jnp.minimum(wide, 0.0)))


def kernel(
    count, q_hbm, k_hbm, v_hbm, g_hbm, w_hbm, out_hbm,
    qb, kb, vb, gb, perm, kh, vh, qh, sig, part, pmass, send1, recv1, chip, cmass, send2, recv2, xsum, xmass,
    send3, recv3, state, mixed, wbuf, outb,
    ld, osem, ya, yb, za, zb, w_send, w_core, s_send, s1, s2, s3, s4, s5,
):
    zh, y, zl, x, core = (lax.axis_index(a) for a in ("zh", "y", "zl", "x", "core"))
    other = 1 - core
    z = 2 * zh + zl
    ds = 2 * zl - 1
    zo, zi = lax.rem(z + ds + 8, 8), lax.rem(z - ds + 8, 8)
    outer = {"zh": zo // 2, "zl": lax.rem(zo, 2)}
    inner = {"zh": zi // 2, "zl": lax.rem(zi, 2)}
    ynext = [{"y": lax.rem(y + 1, 4)}, {"y": lax.rem(y + 3, 4)}]
    xpeer = [{"x": lax.rem(x + d, 4)} for d in (1, 2, 3)]
    partner = {"core": other}

    own = (zh * 4 + y) * SIZE
    wloads = [
        pltpu.make_async_copy(
            w_hbm.at[:, pl.ds(512 * n, 512)], wbuf.at[n, pl.ds(pl.multiple_of(own, SIZE), SIZE), :], ld.at[n]
        )
        for n in range(4)
    ]
    loads = [
        [pltpu.make_async_copy(h.at[s], b.at[s], ld.at[4 + 2 * i + s]) for s in range(SEQS)]
        for i, (h, b) in enumerate(((k_hbm, kb), (v_hbm, vb), (q_hbm, qb), (g_hbm, gb)))
    ]
    for c in wloads:
        c.start()
    for s in range(SEQS):
        loads[0][s].start()
        loads[1][s].start()
    for s in range(SEQS):
        loads[2][s].start()
        loads[3][s].start()

    barrier = pltpu.get_barrier_semaphore()
    for dev in (partner, outer, inner, *ynext, *xpeer):
        pl.semaphore_signal(barrier, inc=1, device_id=dev, device_id_type=MESH)
    row = lax.broadcasted_iota(jnp.int32, (256, 256), 0)
    col = lax.broadcasted_iota(jnp.int32, (256, 256), 1)
    perm[...] = jnp.where(col == (row & 15) * 16 + (row >> 4), 1.0, 0.0).astype(BF16)
    pl.semaphore_wait(barrier, 8)

    def send(src, ssem, rsem, dev, dst=None):
        pltpu.make_async_remote_copy(
            src_ref=src, dst_ref=src if dst is None else dst, send_sem=ssem, recv_sem=rsem,
            device_id=dev, device_id_type=MESH,
        ).start()

    def arrived(ref, rsem):
        pltpu.make_async_copy(ref, ref, rsem).wait()

    def piece(which, zq, yq, half=None):
        at = (lax.rem(zq + 8, 4) * 4 + lax.rem(yq + 8, 4)) * SIZE
        size = SIZE
        if half is not None:
            at, size = at + half * 64, 64
        return wbuf.at[2 * core + which, pl.ds(pl.multiple_of(at, 64), size), :]

    def share(ref):
        send(ref, w_send, w_core, partner)

    def y_full(which, zq, slot):
        ref = piece(which, zq, y)
        for d in range(2):
            send(ref, w_send, ya.at[d, 0, slot], ynext[d])

    def y_got_full(which, zq, slot):
        for d in range(2):
            yq = y - (1 - 2 * d)
            arrived(piece(which, zq, yq), ya.at[d, 0, slot])
            send(piece(which, zq, yq, d), w_send, ya.at[d, 1, slot], ynext[d])
            share(piece(which, zq, yq))

    def y_got_half(which, zq, slot):
        for d in range(2):
            ref = piece(which, zq, y + 2, d)
            arrived(ref, ya.at[d, 1, slot])
            share(ref)

    def z_own(which, yq, slot):
        send(piece(which, zh, yq), w_send, za.at[0, 0, slot], outer)

    def z_outer_full(which, yq, slot):
        ref = piece(which, zh + ds, yq)
        arrived(ref, za.at[0, 0, slot])
        send(ref, w_send, za.at[1, 0, slot], inner)
        share(ref)

    def z_inner_full(which, yq, slot):
        ref = piece(which, zh - ds, yq)
        arrived(ref, za.at[1, 0, slot])
        send(piece(which, zh - ds, yq, 1 - zl), w_send, za.at[0, 1, slot], outer)
        share(ref)

    def z_outer_half(which, yq, slot):
        ref = piece(which, zh + 2, yq, zl)
        arrived(ref, za.at[0, 1, slot])
        send(ref, w_send, za.at[1, 1, slot], inner)
        share(ref)

    def z_inner_half(which, yq, slot):
        ref = piece(which, zh + 2, yq, 1 - zl)
        arrived(ref, za.at[1, 1, slot])
        share(ref)

    for c in wloads:
        c.wait()
    y_full(0, zh, 0)
    z_own(1, y, 4)
    z_own(0, y, 0)
    y_full(1, zh, 1)

    def to_heads(left, right):
        both = jnp.concatenate([left.reshape(256, SIZE), right.reshape(256, SIZE)], axis=1)
        return jnp.dot(perm[...], both, preferred_element_type=F32)

    def sums(s):
        loads[0][s].wait()
        loads[1][s].wait()

        def some(i, mass):
            at = pl.ds(pl.multiple_of(16 * i, 16), 16)
            kf = feature(kb[s, at]).astype(BF16)
            r = to_heads(kf, vb[s, at])
            kh[:, at, :] = r[:, :SIZE].astype(BF16).reshape(HEADS, 16, SIZE)
            vh[:, at, :] = r[:, SIZE:].astype(BF16).reshape(HEADS, 16, SIZE)
            return mass + jnp.sum(kf.astype(F32), axis=0)

        mass = lax.fori_loop(0, 16, some, jnp.zeros((HEADS, SIZE), F32), unroll=2)
        pmass[s] = mass
        send1[s, pl.ds(1024, 16), :] = mass.astype(BF16)

        def one(h):
            return lax.dot_general(vh[h], kh[h], (((0,), (0,)), ((), ())), preferred_element_type=F32)

        def theirs(i, _):
            send1[s, pl.ds(pl.multiple_of(i * SIZE, SIZE), SIZE), :] = one(8 * other + i).astype(BF16)
            return 0

        lax.fori_loop(0, 8, theirs, 0, unroll=2)
        send(send1.at[s], s_send.at[s, 0], s1.at[s], partner, recv1.at[s])

        def ours(i, _):
            part[s, pl.ds(pl.multiple_of(i * SIZE, SIZE), SIZE), :] = one(8 * core + i)
            return 0

        lax.fori_loop(0, 8, ours, 0, unroll=2)

    def chip_sum(s):
        arrived(recv1.at[s], s1.at[s])
        cm = pmass[s] + recv1[s, pl.ds(1024, 16), :].astype(F32)
        cmass[s] = cm

        def group(j, _):
            at = pl.ds(pl.multiple_of(j * 256, 256), 256)
            total = part[s, at, :] + recv1[s, at, :].astype(F32)
            chip[s, at, :] = total
            send2[s, j, pl.ds(0, 256), :] = total.astype(BF16)
            send2[s, j, pl.ds(256, 16), :] = cm.astype(BF16)
            return 0

        lax.fori_loop(0, 4, group, 0)
        for d in range(3):
            send(send2.at[s, lax.rem(x + d + 1, 4)], s_send.at[s, 1 + d], s2.at[s, d], xpeer[d], recv2.at[s, d])

    def x_sum(s):
        for d in range(3):
            arrived(recv2.at[s, d], s2.at[s, d])
        total = chip[s, pl.ds(pl.multiple_of(x * 256, 256), 256), :]
        mass = cmass[s]
        for d in range(3):
            total = total + recv2[s, d, pl.ds(0, 256), :].astype(F32)
            mass = mass + recv2[s, d, pl.ds(256, 16), :].astype(F32)
        xsum[s] = total
        xmass[s] = mass
        send3[s, pl.ds(0, 256), :] = total.astype(BF16)
        send3[s, pl.ds(256, 16), :] = mass.astype(BF16)
        send(send3.at[s], s_send.at[s, 4], s3.at[s], inner, recv3.at[s])

    def blocks(s, c, xq):
        at = (8 * c + 2 * xq) * SIZE
        return state.at[s, pl.ds(pl.multiple_of(at, 256), 256), :]

    def whole_sum(s):
        arrived(recv3.at[s], s3.at[s])
        total = xsum[s] + recv3[s, pl.ds(0, 256), :].astype(F32)
        xmass[s] = (xmass[s] + recv3[s, pl.ds(256, 16), :].astype(F32)) / count
        mine = blocks(s, core, x)
        mine[...] = (total / count).astype(BF16)
        for d in range(3):
            send(mine, s_send.at[s, 5 + d], s4.at[s, d], xpeer[d])
        send(mine, s_send.at[s, 8], s5.at[s, 0], partner)

    def pass_on(s):
        for d in range(3):
            ref = blocks(s, core, lax.rem(x + 3 - d, 4))
            arrived(ref, s4.at[s, d])
            send(ref, s_send.at[s, 9 + d], s5.at[s, 1 + d], partner)

    def all_here(s):
        for d in range(4):
            arrived(blocks(s, other, lax.rem(x + 4 - d, 4)), s5.at[s, d])

    def questions(s):
        loads[2][s].wait()
        loads[3][s].wait()

        def some(i, _):
            at = pl.ds(pl.multiple_of(16 * i, 16), 16)
            r = to_heads(feature(qb[s, at]).astype(BF16), gb[s, at])
            qh[s, :, at, :] = r[:, :SIZE].astype(BF16).reshape(HEADS, 16, SIZE)
            gate = (count**0.5) / (1.0 + jnp.exp(-r[:, SIZE:]))
            sig[s, :, at, :] = gate.reshape(HEADS, 16, SIZE)
            return 0

        lax.fori_loop(0, 16, some, 0, unroll=2)

    def answers(s):
        def one(h, _):
            at = pl.ds(pl.multiple_of(h * SIZE, SIZE), SIZE)
            row = xmass[s, pl.ds(h, 1), :].astype(BF16)
            right = jnp.concatenate([state[s, at, :], jnp.broadcast_to(row, (SIZE, SIZE))], axis=0)
            r = lax.dot_general(qh[s, h], right, (((1,), (1,)), ((), ())), preferred_element_type=F32)
            read = r[:, :SIZE] * sig[s, h] / (r[:, SIZE:] + 0.001)
            mixed[pl.ds(s * ROWS, ROWS), at] = read.astype(BF16)
            return 0

        lax.fori_loop(0, HEADS, one, 0, unroll=2)

    sums(0)
    sums(1)
    y_got_full(0, zh, 0)
    z_own(0, y - 1, 1)
    z_own(0, y + 1, 2)
    z_outer_full(1, y, 4)
    y_full(1, zh + ds, 2)
    chip_sum(0)
    z_outer_full(0, y, 0)
    chip_sum(1)
    y_got_full(1, zh, 1)
    y_got_half(0, zh, 0)
    z_own(0, y + 2, 3)
    z_inner_full(1, y, 4)
    y_full(1, zh - ds, 3)
    questions(0)
    x_sum(0)
    z_inner_full(0, y, 0)
    z_outer_full(0, y - 1, 1)
    z_outer_half(1, y, 4)
    questions(1)
    x_sum(1)
    whole_sum(0)
    z_outer_full(0, y + 1, 2)
    z_inner_full(0, y - 1, 1)
    z_inner_half(1, y, 4)
    y_full(1, zh + 2, 4)
    y_got_full(1, zh + ds, 2)
    y_got_full(1, zh - ds, 3)
    whole_sum(1)
    pass_on(0)
    z_outer_full(0, y + 2, 3)
    z_inner_full(0, y + 1, 2)
    y_got_half(1, zh, 1)
    all_here(0)
    answers(0)
    z_inner_full(0, y + 2, 3)
    y_got_half(1, zh + ds, 2)
    pass_on(1)
    y_got_full(1, zh + 2, 4)
    all_here(1)
    answers(1)
    for slot in range(4):
        z_outer_half(0, y + OFFSETS[slot], slot)
    y_got_half(1, zh - ds, 3)
    for slot in range(4):
        z_inner_half(0, y + OFFSETS[slot], slot)
    y_got_half(1, zh + 2, 4)

    sized = wbuf.at[pl.ds(0, 2), pl.ds(0, 15 * SIZE), :]
    arrived(sized, w_core)

    stores = []
    for n in range(4):
        for s in range(SEQS):
            at = pl.ds(s * ROWS, ROWS)
            o = jnp.dot(mixed[at, :], wbuf[n], preferred_element_type=F32)
            outb[s, :, pl.ds(512 * n, 512)] = o.astype(BF16)
            c = pltpu.make_async_copy(
                outb.at[s, :, pl.ds(512 * n, 512)], out_hbm.at[s, :, pl.ds(512 * n, 512)], osem.at[2 * n + s]
            )
            c.start()
            stores.append(c)

    everything = wbuf.at[:, pl.ds(0, 15 * SIZE), :]
    arrived(everything, w_send)
    for s in range(SEQS):
        arrived(send1.at[s], s_send.at[s, 0])
        for d in range(3):
            arrived(send2.at[s, d], s_send.at[s, 1 + d])
        arrived(send3.at[s], s_send.at[s, 4])
        for d in range(7):
            arrived(blocks(s, core, x), s_send.at[s, 5 + d])
    for c in stores:
        c.wait()


def solution(mesh):
    finer = Mesh(mesh.devices.reshape(4, 4, 2, 4, 2), ("zh", "y", "zl", "x", "core"))
    batch, ctx = ("zh", "y"), ("zl", "x", "core")

    def local(asked_for, offered, contents, gate_rows, out_weight):
        count = float(asked_for.shape[1] * 16)
        dma = pltpu.SemaphoreType.DMA
        vm = pltpu.VMEM
        block = (SEQS, ROWS, HEADS, SIZE)
        return pl.pallas_call(
            lambda *refs: kernel(count, *refs),
            out_shape=jax.ShapeDtypeStruct((SEQS, ROWS, WIDTH), BF16),
            in_specs=[pl.BlockSpec(memory_space=pl.ANY)] * 5,
            out_specs=pl.BlockSpec(memory_space=pl.ANY),
            scratch_shapes=[
                vm(block, BF16), vm(block, BF16), vm(block, BF16), vm(block, BF16),
                vm((256, 256), BF16),
                vm((HEADS, ROWS, SIZE), BF16), vm((HEADS, ROWS, SIZE), BF16),
                vm((SEQS, HEADS, ROWS, SIZE), BF16), vm((SEQS, HEADS, ROWS, SIZE), F32),
                vm((SEQS, 1024, SIZE), F32), vm((SEQS, HEADS, SIZE), F32),
                vm((SEQS, 1040, SIZE), BF16), vm((SEQS, 1040, SIZE), BF16),
                vm((SEQS, 1024, SIZE), F32), vm((SEQS, HEADS, SIZE), F32),
                vm((SEQS, 4, 272, SIZE), BF16), vm((SEQS, 3, 272, SIZE), BF16),
                vm((SEQS, 256, SIZE), F32), vm((SEQS, HEADS, SIZE), F32),
                vm((SEQS, 272, SIZE), BF16), vm((SEQS, 272, SIZE), BF16),
                vm((SEQS, WIDTH, SIZE), BF16),
                vm((SEQS * ROWS, WIDTH), BF16),
                vm((4, WIDTH, 512), BF16),
                vm((SEQS, ROWS, WIDTH), BF16),
                dma((12,)), dma((8,)),
                dma((2, 2, 5)), dma((1,)), dma((2, 2, 5)), dma((1,)),
                dma, dma, dma((SEQS, 12)),
                dma((SEQS,)), dma((SEQS, 3)), dma((SEQS,)), dma((SEQS, 3)), dma((SEQS, 4)),
            ],
            compiler_params=pltpu.CompilerParams(
                collective_id=0, has_side_effects=True, vmem_limit_bytes=60 * 1024 * 1024
            ),
        )(asked_for, offered, contents, gate_rows, out_weight)

    cut = P(batch, ctx, None, None)
    return jax.shard_map(
        local, mesh=finer, in_specs=(cut, cut, cut, cut, P(batch, None)), out_specs=P(batch, ctx, None), check_vma=False
    )
```

```python
import jax
import jax.numpy as jnp
from jax import lax
from jax.experimental import pallas as pl
from jax.experimental.pallas import tpu as pltpu
from jax.sharding import Mesh
from jax.sharding import PartitionSpec as P

F32, BF16 = jnp.float32, jnp.bfloat16
MESH = pl.DeviceIdType.MESH
HEADS, SIZE = 16, 128
SEQS, ROWS = 2, 256
WIDTH = HEADS * SIZE
HALF = SIZE // 2
UN, UK = 8, 4
OFFSETS = (0, 3, 1, 2, 0)
PEERS = (2, 1, 3)


def feature(x):
    wide = x.astype(F32)
    return jnp.where(wide > 0.0, wide + 1.0, jnp.exp(jnp.minimum(wide, 0.0)))


def kernel(
    count, q_hbm, k_hbm, v_hbm, g_hbm, w_hbm, out,
    qb, kb, vb, gb, perm, kh, vh, qh, sig, part, pmass, send1, recv1, chip, send2, recv2, xsum, mass,
    send3, recv3, state, mixed, wbuf,
    ld, ya, za, w_send, w_core, s_send, s1, s2, s3, s4, s5,
):
    zh, y, zl, x, core = (lax.axis_index(a) for a in ("zh", "y", "zl", "x", "core"))
    other = 1 - core
    z = 2 * zh + zl
    ds = 2 * zl - 1
    zo, zi = lax.rem(z + ds + 8, 8), lax.rem(z - ds + 8, 8)
    outer = {"zh": zo // 2, "zl": lax.rem(zo, 2)}
    inner = {"zh": zi // 2, "zl": lax.rem(zi, 2)}
    ynext = [{"y": lax.rem(y + 1, 4)}, {"y": lax.rem(y + 3, 4)}]
    peers = [{"x": lax.rem(x + b, 4)} for b in PEERS]
    partner = {"core": other}

    own = (zh * 4 + y) * SIZE
    wloads = [
        pltpu.make_async_copy(
            w_hbm.at[:, pl.ds(512 * n, 512)], wbuf.at[n, pl.ds(pl.multiple_of(own, SIZE), SIZE), :], ld.at[n]
        )
        for n in range(4)
    ]
    loads = [
        [pltpu.make_async_copy(h.at[s], b.at[s], ld.at[4 + 2 * i + s]) for s in range(SEQS)]
        for i, (h, b) in enumerate(((k_hbm, kb), (v_hbm, vb), (q_hbm, qb), (g_hbm, gb)))
    ]
    for c in wloads:
        c.start()
    for s in range(SEQS):
        loads[0][s].start()
        loads[1][s].start()
    for s in range(SEQS):
        loads[2][s].start()
        loads[3][s].start()

    barrier = pltpu.get_barrier_semaphore()
    for dev in (partner, outer, inner, *ynext, *peers):
        pl.semaphore_signal(barrier, inc=1, device_id=dev, device_id_type=MESH)
    row = lax.broadcasted_iota(jnp.int32, (256, 256), 0)
    col = lax.broadcasted_iota(jnp.int32, (256, 256), 1)
    perm[...] = jnp.where(col == (row & 15) * 16 + (row >> 4), 1.0, 0.0).astype(BF16)
    pl.semaphore_wait(barrier, 8)

    def send(src, ssem, rsem, dev, dst=None):
        pltpu.make_async_remote_copy(
            src_ref=src, dst_ref=src if dst is None else dst, send_sem=ssem, recv_sem=rsem,
            device_id=dev, device_id_type=MESH,
        ).start()

    def arrived(ref, rsem):
        pltpu.make_async_copy(ref, ref, rsem).wait()

    def piece(which, zq, yq, u):
        at = (lax.rem(zq + 8, 4) * 4 + lax.rem(yq + 8, 4)) * SIZE + u * HALF
        return wbuf.at[2 * core + which, pl.ds(pl.multiple_of(at, HALF), HALF), :]

    def share(ref):
        send(ref, w_send, w_core, partner)

    y_zq = (zh, zh, zh + ds, zh - ds, zh + 2)
    y_half = ((0, 1), (0, 1), (zl, 1 - zl), (1 - zl, zl), (zl, 1 - zl))

    def y_send(which, slot, d, u):
        send(piece(which, y_zq[slot], y, u), w_send, ya.at[d, 0, slot, u], ynext[d])

    def y_got_full(which, slot, d, f):
        u = y_half[slot][f]
        ref = piece(which, y_zq[slot], y - (1 - 2 * d), u)
        arrived(ref, ya.at[d, 0, slot, u])

        def onward():
            send(ref, w_send, ya.at[d, 1, slot, 0], ynext[d])

        if slot < 2:
            if u == d:
                onward()
        else:
            pl.when(u == d)(onward)
        share(ref)
        if which == 0:
            z_own(0, 1 + d, u)

    def y_got_half(which, slot, d):
        ref = piece(which, y_zq[slot], y + 2, d)
        arrived(ref, ya.at[d, 1, slot, 0])
        share(ref)
        if which == 0:
            z_own(0, 3, d)

    def z_own(which, slot, u):
        send(piece(which, zh, y + OFFSETS[slot], u), w_send, za.at[0, 0, slot, u], outer)

    def to_y(which, slot, u):
        if which == 1:
            for d in range(2):
                y_send(1, slot, d, u)

    def outer_full(which, slot, f):
        u = (zl, 1 - zl)[f]
        ref = piece(which, zh + ds, y + OFFSETS[slot], u)
        arrived(ref, za.at[0, 0, slot, u])
        send(ref, w_send, za.at[1, 0, slot, u], inner)
        to_y(which, 2, u)
        share(ref)

    def inner_full(which, slot, f):
        u = (1 - zl, zl)[f]
        ref = piece(which, zh - ds, y + OFFSETS[slot], u)
        arrived(ref, za.at[1, 0, slot, u])
        if f == 0:
            send(ref, w_send, za.at[0, 1, slot, 0], outer)
        to_y(which, 3, u)
        share(ref)

    def outer_half(which, slot):
        ref = piece(which, zh + 2, y + OFFSETS[slot], zl)
        arrived(ref, za.at[0, 1, slot, 0])
        send(ref, w_send, za.at[1, 1, slot, 0], inner)
        to_y(which, 4, zl)
        share(ref)

    def inner_half(which, slot):
        ref = piece(which, zh + 2, y + OFFSETS[slot], 1 - zl)
        arrived(ref, za.at[1, 1, slot, 0])
        to_y(which, 4, 1 - zl)
        share(ref)

    for c in wloads:
        c.wait()
    for f in range(2):
        for d in range(2):
            y_send(0, 0, d, (d, 1 - d)[f])
        z_own(1, 4, (1 - zl, zl)[f])
    for f in range(2):
        z_own(0, 0, (1 - zl, zl)[f])
        for d in range(2):
            y_send(1, 1, d, (d, 1 - d)[f])

    def to_heads(left, right):
        both = jnp.concatenate([left.reshape(256, SIZE), right.reshape(256, SIZE)], axis=1)
        return jnp.dot(perm[...], both, preferred_element_type=F32)

    def keys(s, part_of):
        if part_of == 0:
            loads[0][s].wait()
            loads[1][s].wait()

        def some(i, total):
            at = pl.ds(pl.multiple_of(16 * i, 16), 16)
            kf = feature(kb[s, at]).astype(BF16)
            r = to_heads(kf, vb[s, at])
            kh[:, at, :] = r[:, :SIZE].astype(BF16).reshape(HEADS, 16, SIZE)
            vh[:, at, :] = r[:, SIZE:].astype(BF16).reshape(HEADS, 16, SIZE)
            return total + jnp.sum(kf.astype(F32), axis=0)

        start = jnp.zeros((HEADS, SIZE), F32) if part_of == 0 else pmass[s]
        total = lax.fori_loop(8 * part_of, 8 * part_of + 8, some, start, unroll=UK)
        pmass[s] = total
        if part_of == 1:
            send1[s, pl.ds(1024, 16), :] = total.astype(BF16)

    def product(h):
        return lax.dot_general(
            vh[h, pl.ds(0, ROWS), :], kh[h, pl.ds(0, ROWS), :], (((0,), (0,)), ((), ())), preferred_element_type=F32
        )

    def theirs(s):
        def one(i, _):
            send1[s, pl.ds(pl.multiple_of(i * SIZE, SIZE), SIZE), :] = product(8 * other + i).astype(BF16)
            return 0

        lax.fori_loop(0, 8, one, 0, unroll=UN)
        send(send1.at[s], s_send.at[s, 0], s1.at[s], partner, recv1.at[s])

    def ours(s):
        def one(i, _):
            part[s, pl.ds(pl.multiple_of(i * SIZE, SIZE), SIZE), :] = product(8 * core + i)
            return 0

        lax.fori_loop(0, 8, one, 0, unroll=UN)

    def chip_sum(s):
        arrived(recv1.at[s], s1.at[s])
        cm = pmass[s] + recv1[s, pl.ds(1024, 16), :].astype(F32)
        mass[s] = cm

        def one(j, _):
            at = pl.ds(pl.multiple_of(j * 256, 256), 256)
            total = part[s, at, :] + recv1[s, at, :].astype(F32)
            chip[s, at, :] = total
            send2[s, j, pl.ds(0, 256), :] = total.astype(BF16)
            send2[s, j, pl.ds(256, 16), :] = cm.astype(BF16)
            return 0

        lax.fori_loop(0, 4, one, 0)
        for k, b in enumerate(PEERS):
            send(send2.at[s, lax.rem(x + b, 4)], s_send.at[s, 1 + k], s2.at[s, k], peers[k], recv2.at[s, k])

    def pair_of(s, xq):
        return state.at[s, pl.ds(pl.multiple_of((8 * core + 2 * xq) * SIZE, 256), 256), :]

    def x_sum(s):
        total = chip[s, pl.ds(pl.multiple_of(x * 256, 256), 256), :]
        m = mass[s]
        for k in range(3):
            arrived(recv2.at[s, k], s2.at[s, k])
            total = total + recv2[s, k, pl.ds(0, 256), :].astype(F32)
            m = m + recv2[s, k, pl.ds(256, 16), :].astype(F32)
        xsum[s] = total
        mass[s] = m
        send3[s, pl.ds(0, 256), :] = total.astype(BF16)
        send3[s, pl.ds(256, 16), :] = m.astype(BF16)
        send(send3.at[s], s_send.at[s, 4], s3.at[s], inner, recv3.at[s])

    def whole_sum(s):
        arrived(recv3.at[s], s3.at[s])
        mass[s] = (mass[s] + recv3[s, pl.ds(256, 16), :].astype(F32)) / count
        mine = pair_of(s, x)
        mine[...] = ((xsum[s] + recv3[s, pl.ds(0, 256), :].astype(F32)) / count).astype(BF16)
        for k in range(3):
            send(mine, s_send.at[s, 5 + k], s4.at[s, k], peers[k])

    def pass_on(s):
        for k, b in enumerate(PEERS):
            arrived(pair_of(s, lax.rem(x + 4 - b, 4)), s4.at[s, k])
        ref = state.at[s, pl.ds(pl.multiple_of(8 * core * SIZE, SIZE), 8 * SIZE), :]
        send(ref, s_send.at[s, 8], s5.at[s], partner)

    def questions(s, part_of):
        if part_of == 0:
            loads[2][s].wait()
            loads[3][s].wait()

        def some(i, _):
            at = pl.ds(pl.multiple_of(16 * i, 16), 16)
            r = to_heads(feature(qb[s, at]).astype(BF16), gb[s, at])
            qh[s, :, at, :] = r[:, :SIZE].astype(BF16).reshape(HEADS, 16, SIZE)
            gate = (count**0.5) / (1.0 + jnp.exp(-r[:, SIZE:]))
            sig[s, :, at, :] = gate.reshape(HEADS, 16, SIZE)
            return 0

        lax.fori_loop(8 * part_of, 8 * part_of + 8, some, 0, unroll=UK)

    def answers(s, side):
        if side is other:
            arrived(state.at[s, pl.ds(pl.multiple_of(8 * other * SIZE, SIZE), 8 * SIZE), :], s5.at[s])

        def one(i, _):
            h = 8 * side + i
            at = pl.ds(pl.multiple_of(h * SIZE, SIZE), SIZE)
            row = mass[s, pl.ds(h, 1), :].astype(BF16)
            right = jnp.concatenate([state[s, at, :], jnp.broadcast_to(row, (SIZE, SIZE))], axis=0)
            r = lax.dot_general(
                qh[s, h, pl.ds(0, ROWS), :], right, (((1,), (1,)), ((), ())), preferred_element_type=F32
            )
            read = r[:, :SIZE] * sig[s, h, pl.ds(0, ROWS), :] / (r[:, SIZE:] + 0.001)
            mixed[pl.ds(s * ROWS, ROWS), at] = read.astype(BF16)
            return 0

        lax.fori_loop(0, 8, one, 0, unroll=UN)

    keys(0, 0)
    keys(0, 1)
    theirs(0)
    ours(0)
    keys(1, 0)
    keys(1, 1)
    y_got_full(0, 0, 0, 0)
    y_got_full(0, 0, 1, 1)
    outer_full(1, 4, 0)
    chip_sum(0)
    theirs(1)
    ours(1)
    questions(0, 0)
    y_got_full(0, 0, 0, 1)
    y_got_full(0, 0, 1, 0)
    outer_full(1, 4, 1)
    questions(0, 1)
    chip_sum(1)
    questions(1, 0)
    outer_full(0, 0, 0)
    y_got_full(1, 1, 0, 0)
    y_got_full(1, 1, 1, 1)
    questions(1, 1)
    inner_full(1, 4, 0)
    outer_full(0, 0, 1)
    y_got_full(1, 1, 0, 1)
    y_got_full(1, 1, 1, 0)
    inner_full(1, 4, 1)
    y_got_half(0, 0, 0)
    outer_full(0, 1, 0)
    y_got_half(0, 0, 1)
    x_sum(0)
    outer_full(0, 2, 1)
    y_got_full(1, 2, 0, 0)
    y_got_full(1, 2, 1, 0)
    inner_full(0, 0, 0)
    outer_full(0, 1, 1)
    y_got_full(1, 2, 0, 1)
    y_got_full(1, 2, 1, 1)
    inner_full(0, 0, 1)
    x_sum(1)
    outer_full(0, 2, 0)
    y_got_half(1, 1, 0)
    y_got_half(1, 1, 1)
    inner_full(0, 1, 0)
    outer_half(1, 4)
    y_got_full(1, 3, 0, 0)
    y_got_full(1, 3, 1, 0)
    whole_sum(0)
    y_got_full(1, 3, 0, 1)
    y_got_full(1, 3, 1, 1)
    outer_full(0, 3, 0)
    inner_full(0, 2, 1)
    outer_full(0, 3, 1)
    y_got_half(1, 2, 0)
    y_got_half(1, 2, 1)
    inner_full(0, 1, 1)
    outer_half(0, 0)
    y_got_full(1, 4, 0, 0)
    y_got_full(1, 4, 1, 0)
    whole_sum(1)
    outer_half(0, 1)
    y_got_half(1, 3, 0)
    y_got_half(1, 3, 1)
    inner_full(0, 2, 0)
    pass_on(0)
    answers(0, core)
    inner_half(1, 4)
    answers(0, other)
    inner_full(0, 3, 0)
    outer_half(0, 2)
    inner_full(0, 3, 1)
    pass_on(1)
    answers(1, core)
    y_got_full(1, 4, 0, 1)
    y_got_full(1, 4, 1, 1)
    inner_half(0, 0)
    answers(1, other)
    outer_half(0, 3)
    inner_half(0, 1)
    inner_half(0, 2)
    y_got_half(1, 4, 0)
    y_got_half(1, 4, 1)
    inner_half(0, 3)

    def project(n, s):
        o = jnp.dot(mixed[pl.ds(s * ROWS, ROWS), :], wbuf[n], preferred_element_type=F32)
        at = pl.ds(pl.multiple_of(512 * n, 512), 512)
        out[s, :, at] = o.astype(BF16)

    for i in range(2):
        for s in range(SEQS):
            project(2 * core + i, s)
    arrived(wbuf.at[pl.ds(0, 2), pl.ds(0, 15 * SIZE), :], w_core)
    for i in range(2):
        for s in range(SEQS):
            project(2 * other + i, s)

    arrived(wbuf.at[:, pl.ds(0, 15 * SIZE), :], w_send)
    for s in range(SEQS):
        arrived(send1.at[s], s_send.at[s, 0])
        for k in range(3):
            arrived(send2.at[s, 0], s_send.at[s, 1 + k])
            arrived(pair_of(s, x), s_send.at[s, 5 + k])
        arrived(send3.at[s], s_send.at[s, 4])
        arrived(state.at[s, pl.ds(0, 8 * SIZE), :], s_send.at[s, 8])


def solution(mesh):
    finer = Mesh(mesh.devices.reshape(4, 4, 2, 4, 2), ("zh", "y", "zl", "x", "core"))
    batch, ctx = ("zh", "y"), ("zl", "x", "core")

    def local(asked_for, offered, contents, gate_rows, out_weight):
        count = float(asked_for.shape[1] * 16)
        dma = pltpu.SemaphoreType.DMA
        vm = pltpu.VMEM
        block = (SEQS, ROWS, HEADS, SIZE)
        return pl.pallas_call(
            lambda *refs: kernel(count, *refs),
            out_shape=jax.ShapeDtypeStruct((SEQS, ROWS, WIDTH), BF16),
            in_specs=[pl.BlockSpec(memory_space=pltpu.HBM)] * 5,
            out_specs=pl.BlockSpec(memory_space=pltpu.VMEM),
            scratch_shapes=[
                vm(block, BF16), vm(block, BF16), vm(block, BF16), vm(block, BF16),
                vm((256, 256), BF16),
                vm((HEADS, ROWS + 16, SIZE), BF16), vm((HEADS, ROWS + 16, SIZE), BF16),
                vm((SEQS, HEADS, ROWS + 16, SIZE), BF16), vm((SEQS, HEADS, ROWS + 8, SIZE), F32),
                vm((SEQS, 1024, SIZE), F32), vm((SEQS, HEADS, SIZE), F32),
                vm((SEQS, 1040, SIZE), BF16), vm((SEQS, 1040, SIZE), BF16),
                vm((SEQS, 1024, SIZE), F32),
                vm((SEQS, 4, 272, SIZE), BF16), vm((SEQS, 3, 272, SIZE), BF16),
                vm((SEQS, 256, SIZE), F32), vm((SEQS, HEADS, SIZE), F32),
                vm((SEQS, 272, SIZE), BF16), vm((SEQS, 272, SIZE), BF16),
                vm((SEQS, WIDTH, SIZE), BF16),
                vm((SEQS * ROWS, WIDTH), BF16),
                vm((4, WIDTH, 512), BF16),
                dma((12,)),
                dma((2, 2, 5, 2)), dma((2, 2, 5, 2)),
                dma, dma, dma((SEQS, 9)),
                dma((SEQS,)), dma((SEQS, 3)), dma((SEQS,)), dma((SEQS, 3)), dma((SEQS,)),
            ],
            compiler_params=pltpu.CompilerParams(
                collective_id=0, has_side_effects=True, vmem_limit_bytes=44 * 1024 * 1024
            ),
        )(*(pltpu.with_memory_space_constraint(a, pltpu.HBM) for a in (asked_for, offered, contents, gate_rows, out_weight)))

    cut = P(batch, ctx, None, None)
    return jax.shard_map(
        local, mesh=finer, in_specs=(cut, cut, cut, cut, P(batch, None)), out_specs=P(batch, ctx, None), check_vma=False
    )
```

```python
import jax
import jax.numpy as jnp
from jax import lax
from jax.experimental import pallas as pl
from jax.experimental.pallas import tpu as pltpu
from jax.sharding import Mesh
from jax.sharding import PartitionSpec as P

F32, BF16 = jnp.float32, jnp.bfloat16
MESH = pl.DeviceIdType.MESH
HEADS, SIZE = 16, 128
SEQS, ROWS = 2, 256
WIDTH = HEADS * SIZE
HALF = SIZE // 2
CUT = 384
UN, UK = 8, 4
OFFSETS = (0, 3, 1, 2, 0)
PEERS = (2, 1, 3)


def feature(x):
    wide = x.astype(F32)
    return jnp.where(wide > 0.0, wide + 1.0, jnp.exp(jnp.minimum(wide, 0.0)))


def kernel(
    count, q_hbm, k_hbm, v_hbm, g_hbm, w_hbm, out,
    qb, kb, vb, gb, perm, kh, vh, qh, sig, part, pmass, send1, recv1, chip, send2, recv2, xsum, mass,
    send3, recv3, state, mixed, wa, wb, acca, accb,
    ld, ya, za, w_send, w_core, s_send, s1, s2, s3, s4, s5,
):
    zh, y, zl, x, core = (lax.axis_index(a) for a in ("zh", "y", "zl", "x", "core"))
    other = 1 - core
    z = 2 * zh + zl
    ds = 2 * zl - 1
    zo, zi = lax.rem(z + ds + 8, 8), lax.rem(z - ds + 8, 8)
    outer = {"zh": zo // 2, "zl": lax.rem(zo, 2)}
    inner = {"zh": zi // 2, "zl": lax.rem(zi, 2)}
    ynext = [{"y": lax.rem(y + 1, 4)}, {"y": lax.rem(y + 3, 4)}]
    peers = [{"x": lax.rem(x + b, 4)} for b in PEERS]
    partner = {"core": other}

    own = (zh * 4 + y) * SIZE
    wbuf, acc = (wa, wb), (acca, accb)
    block_cols = ((0, CUT), (CUT, 1024 - CUT))
    wloads = [
        pltpu.make_async_copy(
            w_hbm.at[:, pl.ds(1024 * c + block_cols[which][0], block_cols[which][1])],
            wbuf[which].at[c, pl.ds(pl.multiple_of(own, SIZE), SIZE), :],
            ld.at[2 * c + which],
        )
        for which in range(2)
        for c in range(2)
    ]
    loads = [
        [pltpu.make_async_copy(h.at[s], b.at[s], ld.at[4 + 2 * i + s]) for s in range(SEQS)]
        for i, (h, b) in enumerate(((k_hbm, kb), (v_hbm, vb), (q_hbm, qb), (g_hbm, gb)))
    ]
    for c in wloads:
        c.start()
    for s in range(SEQS):
        loads[0][s].start()
        loads[1][s].start()
    for s in range(SEQS):
        loads[2][s].start()
        loads[3][s].start()

    barrier = pltpu.get_barrier_semaphore()
    for dev in (partner, outer, inner, *ynext, *peers):
        pl.semaphore_signal(barrier, inc=1, device_id=dev, device_id_type=MESH)
    row = lax.broadcasted_iota(jnp.int32, (256, 256), 0)
    col = lax.broadcasted_iota(jnp.int32, (256, 256), 1)
    perm[...] = jnp.where(col == (row & 15) * 16 + (row >> 4), 1.0, 0.0).astype(BF16)
    pl.semaphore_wait(barrier, 8)

    def send(src, ssem, rsem, dev, dst=None):
        pltpu.make_async_remote_copy(
            src_ref=src, dst_ref=src if dst is None else dst, send_sem=ssem, recv_sem=rsem,
            device_id=dev, device_id_type=MESH,
        ).start()

    def arrived(ref, rsem):
        pltpu.make_async_copy(ref, ref, rsem).wait()

    def piece(which, zq, yq, u):
        at = (lax.rem(zq + 8, 4) * 4 + lax.rem(yq + 8, 4)) * SIZE + u * HALF
        return wbuf[which].at[core, pl.ds(pl.multiple_of(at, HALF), HALF), :]

    def share(ref, which, group):
        send(ref, w_send.at[which], w_core.at[which, group], partner)

    y_zq = (zh, zh, zh + ds, zh - ds, zh + 2)
    y_half = ((0, 1), (0, 1), (zl, 1 - zl), (1 - zl, zl), (zl, 1 - zl))

    def y_send(which, slot, d, u):
        send(piece(which, y_zq[slot], y, u), w_send.at[which], ya.at[d, 0, slot, u], ynext[d])

    def y_got_full(which, slot, d, f):
        u = y_half[slot][f]
        ref = piece(which, y_zq[slot], y - (1 - 2 * d), u)
        arrived(ref, ya.at[d, 0, slot, u])

        def onward():
            send(ref, w_send.at[which], ya.at[d, 1, slot, 0], ynext[d])

        if slot < 2:
            if u == d:
                onward()
        else:
            pl.when(u == d)(onward)
        share(ref, which, (0, 0, 1, 2, 3)[slot])
        if which == 0:
            z_own(0, 1 + d, u)

    def y_got_half(which, slot, d):
        ref = piece(which, y_zq[slot], y + 2, d)
        arrived(ref, ya.at[d, 1, slot, 0])
        share(ref, which, (0, 0, 1, 2, 3)[slot])
        if which == 0:
            z_own(0, 3, d)

    def z_own(which, slot, u):
        send(piece(which, zh, y + OFFSETS[slot], u), w_send.at[which], za.at[0, 0, slot, u], outer)

    def to_y(which, slot, u):
        if which == 1:
            for d in range(2):
                y_send(1, slot, d, u)

    def outer_full(which, slot, f):
        u = (zl, 1 - zl)[f]
        ref = piece(which, zh + ds, y + OFFSETS[slot], u)
        arrived(ref, za.at[0, 0, slot, u])
        send(ref, w_send.at[which], za.at[1, 0, slot, u], inner)
        to_y(which, 2, u)
        share(ref, which, 1)

    def inner_full(which, slot, f):
        u = (1 - zl, zl)[f]
        ref = piece(which, zh - ds, y + OFFSETS[slot], u)
        arrived(ref, za.at[1, 0, slot, u])
        if f == 0:
            send(ref, w_send.at[which], za.at[0, 1, slot, 0], outer)
        to_y(which, 3, u)
        share(ref, which, 2)

    def outer_half(which, slot):
        ref = piece(which, zh + 2, y + OFFSETS[slot], zl)
        arrived(ref, za.at[0, 1, slot, 0])
        send(ref, w_send.at[which], za.at[1, 1, slot, 0], inner)
        to_y(which, 4, zl)
        share(ref, which, 3)

    def inner_half(which, slot):
        ref = piece(which, zh + 2, y + OFFSETS[slot], 1 - zl)
        arrived(ref, za.at[1, 1, slot, 0])
        to_y(which, 4, 1 - zl)
        share(ref, which, 3)

    for c in wloads:
        c.wait()
    for f in range(2):
        for d in range(2):
            y_send(0, 0, d, (d, 1 - d)[f])
        z_own(1, 4, (1 - zl, zl)[f])
    for f in range(2):
        z_own(0, 0, (1 - zl, zl)[f])
        for d in range(2):
            y_send(1, 1, d, (d, 1 - d)[f])

    def to_heads(left, right):
        both = jnp.concatenate([left.reshape(256, SIZE), right.reshape(256, SIZE)], axis=1)
        return jnp.dot(perm[...], both, preferred_element_type=F32)

    def keys(s, part_of):
        if part_of == 0:
            loads[0][s].wait()
            loads[1][s].wait()

        def some(i, total):
            at = pl.ds(pl.multiple_of(16 * i, 16), 16)
            kf = feature(kb[s, at]).astype(BF16)
            r = to_heads(kf, vb[s, at])
            kh[:, at, :] = r[:, :SIZE].astype(BF16).reshape(HEADS, 16, SIZE)
            vh[:, at, :] = r[:, SIZE:].astype(BF16).reshape(HEADS, 16, SIZE)
            return total + jnp.sum(kf.astype(F32), axis=0)

        start = jnp.zeros((HEADS, SIZE), F32) if part_of == 0 else pmass[s]
        total = lax.fori_loop(8 * part_of, 8 * part_of + 8, some, start, unroll=UK)
        pmass[s] = total
        if part_of == 1:
            send1[s, pl.ds(1024, 16), :] = total.astype(BF16)

    def product(h):
        return lax.dot_general(
            vh[h, pl.ds(0, ROWS), :], kh[h, pl.ds(0, ROWS), :], (((0,), (0,)), ((), ())), preferred_element_type=F32
        )

    def theirs(s):
        def one(i, _):
            send1[s, pl.ds(pl.multiple_of(i * SIZE, SIZE), SIZE), :] = product(8 * other + i).astype(BF16)
            return 0

        lax.fori_loop(0, 8, one, 0, unroll=UN)
        send(send1.at[s], s_send.at[s, 0], s1.at[s], partner, recv1.at[s])

    def ours(s):
        def one(i, _):
            part[s, pl.ds(pl.multiple_of(i * SIZE, SIZE), SIZE), :] = product(8 * core + i)
            return 0

        lax.fori_loop(0, 8, one, 0, unroll=UN)

    def chip_sum(s):
        arrived(recv1.at[s], s1.at[s])
        cm = pmass[s] + recv1[s, pl.ds(1024, 16), :].astype(F32)
        mass[s] = cm

        def one(j, _):
            at = pl.ds(pl.multiple_of(j * 256, 256), 256)
            total = part[s, at, :] + recv1[s, at, :].astype(F32)
            chip[s, at, :] = total
            send2[s, j, pl.ds(0, 256), :] = total.astype(BF16)
            send2[s, j, pl.ds(256, 16), :] = cm.astype(BF16)
            return 0

        lax.fori_loop(0, 4, one, 0)
        for k, b in enumerate(PEERS):
            send(send2.at[s, lax.rem(x + b, 4)], s_send.at[s, 1 + k], s2.at[s, k], peers[k], recv2.at[s, k])

    def pair_of(s, xq):
        return state.at[s, pl.ds(pl.multiple_of((8 * core + 2 * xq) * SIZE, 256), 256), :]

    def x_sum(s):
        total = chip[s, pl.ds(pl.multiple_of(x * 256, 256), 256), :]
        m = mass[s]
        for k in range(3):
            arrived(recv2.at[s, k], s2.at[s, k])
            total = total + recv2[s, k, pl.ds(0, 256), :].astype(F32)
            m = m + recv2[s, k, pl.ds(256, 16), :].astype(F32)
        xsum[s] = total
        mass[s] = m
        send3[s, pl.ds(0, 256), :] = total.astype(BF16)
        send3[s, pl.ds(256, 16), :] = m.astype(BF16)
        send(send3.at[s], s_send.at[s, 4], s3.at[s], inner, recv3.at[s])

    def whole_sum(s):
        arrived(recv3.at[s], s3.at[s])
        mass[s] = (mass[s] + recv3[s, pl.ds(256, 16), :].astype(F32)) / count
        mine = pair_of(s, x)
        mine[...] = ((xsum[s] + recv3[s, pl.ds(0, 256), :].astype(F32)) / count).astype(BF16)
        for k in range(3):
            send(mine, s_send.at[s, 5 + k], s4.at[s, k], peers[k])

    def pass_on(s):
        for k, b in enumerate(PEERS):
            arrived(pair_of(s, lax.rem(x + 4 - b, 4)), s4.at[s, k])
        ref = state.at[s, pl.ds(pl.multiple_of(8 * core * SIZE, SIZE), 8 * SIZE), :]
        send(ref, s_send.at[s, 8], s5.at[s], partner)

    def questions(s, part_of):
        if part_of == 0:
            loads[2][s].wait()
            loads[3][s].wait()

        def some(i, _):
            at = pl.ds(pl.multiple_of(16 * i, 16), 16)
            r = to_heads(feature(qb[s, at]).astype(BF16), gb[s, at])
            qh[s, :, at, :] = r[:, :SIZE].astype(BF16).reshape(HEADS, 16, SIZE)
            gate = (count**0.5) / (1.0 + jnp.exp(-r[:, SIZE:]))
            sig[s, :, at, :] = gate.reshape(HEADS, 16, SIZE)
            return 0

        lax.fori_loop(8 * part_of, 8 * part_of + 8, some, 0, unroll=UK)

    def answers(s, side):
        if side is other:
            arrived(state.at[s, pl.ds(pl.multiple_of(8 * other * SIZE, SIZE), 8 * SIZE), :], s5.at[s])

        def one(i, _):
            h = 8 * side + i
            at = pl.ds(pl.multiple_of(h * SIZE, SIZE), SIZE)
            row = mass[s, pl.ds(h, 1), :].astype(BF16)
            right = jnp.concatenate([state[s, at, :], jnp.broadcast_to(row, (SIZE, SIZE))], axis=0)
            r = lax.dot_general(
                qh[s, h, pl.ds(0, ROWS), :], right, (((1,), (1,)), ((), ())), preferred_element_type=F32
            )
            read = r[:, :SIZE] * sig[s, h, pl.ds(0, ROWS), :] / (r[:, SIZE:] + 0.001)
            mixed[pl.ds(s * ROWS, ROWS), at] = read.astype(BF16)
            return 0

        lax.fori_loop(0, 8, one, 0, unroll=UN)

    def project(group, side):
        groups = (0, 1, 2) if group == 2 else (3,)
        for which in range(2):
            if side is other:
                for g in groups:
                    arrived(wbuf[which].at[0, pl.ds(0, 512 if g else 384), :], w_core.at[which, g])
            off, cols = block_cols[which]
            for s in range(SEQS):
                at = pl.ds(s * ROWS, ROWS)
                o = None if group == 2 else acc[which][side, at, :]
                for g in groups:
                    zq = lax.rem((zh, zh + ds, zh - ds, zh + 2)[g] + 4, 4)
                    rows = pl.ds(pl.multiple_of(zq * 512, 512), 512)
                    part_of = jnp.dot(mixed[at, rows], wbuf[which][side, rows, :], preferred_element_type=F32)
                    o = part_of if o is None else o + part_of
                if group == 2:
                    acc[which][side, at, :] = o
                else:
                    out[s, :, pl.ds(pl.multiple_of(1024 * side + off, SIZE), cols)] = o.astype(BF16)

    keys(0, 0)
    keys(0, 1)
    theirs(0)
    ours(0)
    keys(1, 0)
    chip_sum(0)
    y_got_full(0, 0, 0, 0)
    y_got_full(0, 0, 1, 1)
    keys(1, 1)
    outer_full(1, 4, 0)
    y_got_full(0, 0, 0, 1)
    theirs(1)
    y_got_full(0, 0, 1, 0)
    ours(1)
    outer_full(1, 4, 1)
    chip_sum(1)
    questions(1, 0)
    questions(0, 0)
    y_got_full(1, 1, 1, 1)
    outer_full(0, 0, 0)
    y_got_full(1, 1, 1, 0)
    inner_full(1, 4, 0)
    y_got_half(0, 0, 1)
    x_sum(0)
    inner_full(1, 4, 1)
    y_got_half(0, 0, 0)
    outer_full(0, 1, 0)
    y_got_full(1, 2, 0, 1)
    y_got_full(1, 1, 0, 1)
    x_sum(1)
    inner_full(0, 0, 0)
    whole_sum(0)
    outer_half(1, 4)
    y_got_full(1, 3, 1, 0)
    outer_full(0, 3, 0)
    outer_full(0, 2, 0)
    y_got_full(1, 3, 0, 0)
    y_got_full(1, 3, 0, 1)
    outer_full(0, 1, 1)
    outer_full(0, 0, 1)
    whole_sum(1)
    outer_full(0, 3, 1)
    questions(0, 1)
    y_got_full(1, 2, 0, 0)
    y_got_full(1, 2, 1, 1)
    y_got_full(1, 2, 1, 0)
    inner_full(0, 1, 0)
    y_got_half(1, 1, 1)
    inner_half(1, 4)
    pass_on(0)
    y_got_full(1, 4, 1, 0)
    questions(1, 1)
    outer_full(0, 2, 1)
    inner_full(0, 3, 0)
    outer_half(0, 0)
    y_got_half(1, 3, 0)
    y_got_full(1, 3, 1, 1)
    y_got_full(1, 1, 0, 0)
    answers(0, other)
    inner_full(0, 2, 0)
    pass_on(1)
    outer_half(0, 1)
    y_got_half(1, 2, 1)
    y_got_half(1, 2, 0)
    y_got_full(1, 4, 0, 1)
    y_got_full(1, 4, 1, 1)
    outer_half(0, 3)
    y_got_full(1, 4, 0, 0)
    answers(1, other)
    inner_full(0, 1, 1)
    answers(1, core)
    answers(0, core)
    inner_full(0, 3, 1)
    outer_half(0, 2)
    y_got_half(1, 3, 1)
    inner_full(0, 0, 1)
    inner_full(0, 2, 1)
    y_got_half(1, 1, 0)
    project(2, core)
    inner_half(0, 0)
    project(2, other)
    y_got_half(1, 4, 0)
    y_got_half(1, 4, 1)
    inner_half(0, 3)
    inner_half(0, 2)
    inner_half(0, 1)
    project(3, core)
    project(3, other)

    for which in range(2):
        arrived(wbuf[which].at[:, pl.ds(0, 15 * SIZE), :], w_send.at[which])
    for s in range(SEQS):
        arrived(send1.at[s], s_send.at[s, 0])
        for k in range(3):
            arrived(send2.at[s, 0], s_send.at[s, 1 + k])
            arrived(pair_of(s, x), s_send.at[s, 5 + k])
        arrived(send3.at[s], s_send.at[s, 4])
        arrived(state.at[s, pl.ds(0, 8 * SIZE), :], s_send.at[s, 8])


def solution(mesh):
    finer = Mesh(mesh.devices.reshape(4, 4, 2, 4, 2), ("zh", "y", "zl", "x", "core"))
    batch, ctx = ("zh", "y"), ("zl", "x", "core")

    def local(asked_for, offered, contents, gate_rows, out_weight):
        count = float(asked_for.shape[1] * 16)
        dma = pltpu.SemaphoreType.DMA
        vm = pltpu.VMEM
        block = (SEQS, ROWS, HEADS, SIZE)
        return pl.pallas_call(
            lambda *refs: kernel(count, *refs),
            out_shape=jax.ShapeDtypeStruct((SEQS, ROWS, WIDTH), BF16),
            in_specs=[pl.BlockSpec(memory_space=pltpu.HBM)] * 5,
            out_specs=pl.BlockSpec(memory_space=pltpu.VMEM),
            scratch_shapes=[
                vm(block, BF16), vm(block, BF16), vm(block, BF16), vm(block, BF16),
                vm((256, 256), BF16),
                vm((HEADS, ROWS + 16, SIZE), BF16), vm((HEADS, ROWS + 16, SIZE), BF16),
                vm((SEQS, HEADS, ROWS + 16, SIZE), BF16), vm((SEQS, HEADS, ROWS + 8, SIZE), F32),
                vm((SEQS, 1024, SIZE), F32), vm((SEQS, HEADS, SIZE), F32),
                vm((SEQS, 1040, SIZE), BF16), vm((SEQS, 1040, SIZE), BF16),
                vm((SEQS, 1024, SIZE), F32),
                vm((SEQS, 4, 272, SIZE), BF16), vm((SEQS, 3, 272, SIZE), BF16),
                vm((SEQS, 256, SIZE), F32), vm((SEQS, HEADS, SIZE), F32),
                vm((SEQS, 272, SIZE), BF16), vm((SEQS, 272, SIZE), BF16),
                vm((SEQS, WIDTH, SIZE), BF16),
                vm((SEQS * ROWS, WIDTH), BF16),
                vm((2, WIDTH, CUT), BF16), vm((2, WIDTH, 1024 - CUT), BF16),
                vm((2, SEQS * ROWS, CUT), F32), vm((2, SEQS * ROWS, 1024 - CUT), F32),
                dma((12,)),
                dma((2, 2, 5, 2)), dma((2, 2, 5, 2)),
                dma((2,)), dma((2, 4)), dma((SEQS, 9)),
                dma((SEQS,)), dma((SEQS, 3)), dma((SEQS,)), dma((SEQS, 3)), dma((SEQS,)),
            ],
            compiler_params=pltpu.CompilerParams(
                collective_id=0, has_side_effects=True, vmem_limit_bytes=48 * 1024 * 1024
            ),
        )(*(pltpu.with_memory_space_constraint(a, pltpu.HBM) for a in (asked_for, offered, contents, gate_rows, out_weight)))

    cut = P(batch, ctx, None, None)
    return jax.shard_map(
        local, mesh=finer, in_specs=(cut, cut, cut, cut, P(batch, None)), out_specs=P(batch, ctx, None), check_vma=False
    )
```

```python
import jax
import jax.numpy as jnp
from jax import lax
from jax.experimental import pallas as pl
from jax.experimental.pallas import tpu as pltpu
from jax.sharding import Mesh
from jax.sharding import PartitionSpec as P

F32, BF16 = jnp.float32, jnp.bfloat16
MESH = pl.DeviceIdType.MESH
HEADS, SIZE = 16, 128
SEQS, ROWS = 2, 256
WIDTH = HEADS * SIZE
HALF = SIZE // 2
CUT = 384
UN, UK = 8, 4
OFFSETS = (0, 3, 1, 2, 0)
PEERS = (2, 1, 3)


def feature(x):
    wide = x.astype(F32)
    return jnp.where(wide > 0.0, wide + 1.0, jnp.exp(jnp.minimum(wide, 0.0)))


def kernel(
    count, q_hbm, k_hbm, v_hbm, g_hbm, w_hbm, out,
    qb, kb, vb, gb, perm, kh, vh, qh, sig, part, pmass, send1, recv1, chip, send2, recv2, xsum, mass,
    send3, recv3, state, mixed, wa, wb, acca, accb,
    ld, ya, za, w_send, w_core, s_send, s1, s2, s3, s4, s5,
):
    zh, y, zl, x, core = (lax.axis_index(a) for a in ("zh", "y", "zl", "x", "core"))
    other = 1 - core
    z = 2 * zh + zl
    ds = 2 * zl - 1
    zo, zi = lax.rem(z + ds + 8, 8), lax.rem(z - ds + 8, 8)
    outer = {"zh": zo // 2, "zl": lax.rem(zo, 2)}
    inner = {"zh": zi // 2, "zl": lax.rem(zi, 2)}
    ynext = [{"y": lax.rem(y + 1, 4)}, {"y": lax.rem(y + 3, 4)}]
    peers = [{"x": lax.rem(x + b, 4)} for b in PEERS]
    partner = {"core": other}

    own = (zh * 4 + y) * SIZE
    wbuf, acc = (wa, wb), (acca, accb)
    block_cols = ((0, CUT), (CUT, 1024 - CUT))
    wloads = [
        pltpu.make_async_copy(
            w_hbm.at[:, pl.ds(1024 * c + block_cols[which][0], block_cols[which][1])],
            wbuf[which].at[c, pl.ds(pl.multiple_of(own, SIZE), SIZE), :],
            ld.at[2 * c + which],
        )
        for which in range(2)
        for c in range(2)
    ]
    loads = [
        [pltpu.make_async_copy(h.at[s], b.at[s], ld.at[4 + 2 * i + s]) for s in range(SEQS)]
        for i, (h, b) in enumerate(((k_hbm, kb), (v_hbm, vb), (q_hbm, qb), (g_hbm, gb)))
    ]
    for c in wloads:
        c.start()
    for s in range(SEQS):
        loads[0][s].start()
        loads[1][s].start()
    for s in range(SEQS):
        loads[2][s].start()
        loads[3][s].start()

    barrier = pltpu.get_barrier_semaphore()
    for dev in (partner, outer, inner, *ynext, *peers):
        pl.semaphore_signal(barrier, inc=1, device_id=dev, device_id_type=MESH)
    row = lax.broadcasted_iota(jnp.int32, (256, 256), 0)
    col = lax.broadcasted_iota(jnp.int32, (256, 256), 1)
    perm[...] = jnp.where(col == (row & 15) * 16 + (row >> 4), 1.0, 0.0).astype(BF16)
    pl.semaphore_wait(barrier, 8)

    def send(src, ssem, rsem, dev, dst=None):
        pltpu.make_async_remote_copy(
            src_ref=src, dst_ref=src if dst is None else dst, send_sem=ssem, recv_sem=rsem,
            device_id=dev, device_id_type=MESH,
        ).start()

    def arrived(ref, rsem):
        pltpu.make_async_copy(ref, ref, rsem).wait()

    def piece(which, zq, yq, u):
        at = (lax.rem(zq + 8, 4) * 4 + lax.rem(yq + 8, 4)) * SIZE + u * HALF
        return wbuf[which].at[core, pl.ds(pl.multiple_of(at, HALF), HALF), :]

    def share(ref, which, group):
        send(ref, w_send.at[which], w_core.at[which, group], partner)

    y_zq = (zh, zh, zh + ds, zh - ds, zh + 2)
    y_half = ((0, 1), (0, 1), (zl, 1 - zl), (1 - zl, zl), (zl, 1 - zl))

    def y_send(which, slot, d, u):
        send(piece(which, y_zq[slot], y, u), w_send.at[which], ya.at[d, 0, slot, u], ynext[d])

    def y_got_full(which, slot, d, f):
        u = y_half[slot][f]
        ref = piece(which, y_zq[slot], y - (1 - 2 * d), u)
        arrived(ref, ya.at[d, 0, slot, u])

        def onward():
            send(ref, w_send.at[which], ya.at[d, 1, slot, 0], ynext[d])

        if slot < 2:
            if u == d:
                onward()
        else:
            pl.when(u == d)(onward)
        share(ref, which, (0, 0, 1, 2, 3)[slot])
        if which == 0:
            z_own(0, 1 + d, u)

    def y_got_half(which, slot, d):
        ref = piece(which, y_zq[slot], y + 2, d)
        arrived(ref, ya.at[d, 1, slot, 0])
        share(ref, which, (0, 0, 1, 2, 3)[slot])
        if which == 0:
            z_own(0, 3, d)

    def z_own(which, slot, u):
        send(piece(which, zh, y + OFFSETS[slot], u), w_send.at[which], za.at[0, 0, slot, u], outer)

    def to_y(which, slot, u):
        if which == 1:
            for d in range(2):
                y_send(1, slot, d, u)

    def outer_full(which, slot, f):
        u = (zl, 1 - zl)[f]
        ref = piece(which, zh + ds, y + OFFSETS[slot], u)
        arrived(ref, za.at[0, 0, slot, u])
        send(ref, w_send.at[which], za.at[1, 0, slot, u], inner)
        to_y(which, 2, u)
        share(ref, which, 1)

    def inner_full(which, slot, f):
        u = (1 - zl, zl)[f]
        ref = piece(which, zh - ds, y + OFFSETS[slot], u)
        arrived(ref, za.at[1, 0, slot, u])
        if f == 0:
            send(ref, w_send.at[which], za.at[0, 1, slot, 0], outer)
        to_y(which, 3, u)
        share(ref, which, 2)

    def outer_half(which, slot):
        ref = piece(which, zh + 2, y + OFFSETS[slot], zl)
        arrived(ref, za.at[0, 1, slot, 0])
        send(ref, w_send.at[which], za.at[1, 1, slot, 0], inner)
        to_y(which, 4, zl)
        share(ref, which, 3)

    def inner_half(which, slot):
        ref = piece(which, zh + 2, y + OFFSETS[slot], 1 - zl)
        arrived(ref, za.at[1, 1, slot, 0])
        to_y(which, 4, 1 - zl)
        share(ref, which, 3)

    for c in wloads:
        c.wait()
    for f in range(2):
        for d in range(2):
            y_send(0, 0, d, (d, 1 - d)[f])
        z_own(1, 4, (1 - zl, zl)[f])
    for f in range(2):
        z_own(0, 0, (1 - zl, zl)[f])
        for d in range(2):
            y_send(1, 1, d, (d, 1 - d)[f])

    def to_heads(left, right):
        both = jnp.concatenate([left.reshape(256, SIZE), right.reshape(256, SIZE)], axis=1)
        return jnp.dot(perm[...], both, preferred_element_type=F32)

    def keys(s, part_of):
        if part_of == 0:
            loads[0][s].wait()
            loads[1][s].wait()

        def some(i, total):
            at = pl.ds(pl.multiple_of(16 * i, 16), 16)
            kf = feature(kb[s, at]).astype(BF16)
            r = to_heads(kf, vb[s, at])
            kh[:, at, :] = r[:, :SIZE].astype(BF16).reshape(HEADS, 16, SIZE)
            vh[:, at, :] = r[:, SIZE:].astype(BF16).reshape(HEADS, 16, SIZE)
            return total + jnp.sum(kf.astype(F32), axis=0)

        start = jnp.zeros((HEADS, SIZE), F32) if part_of == 0 else pmass[s]
        total = lax.fori_loop(8 * part_of, 8 * part_of + 8, some, start, unroll=UK)
        pmass[s] = total
        if part_of == 1:
            send1[s, pl.ds(1024, 16), :] = total.astype(BF16)

    def product(h):
        return lax.dot_general(
            vh[h, pl.ds(0, ROWS), :], kh[h, pl.ds(0, ROWS), :], (((0,), (0,)), ((), ())), preferred_element_type=F32
        )

    def theirs(s):
        def one(i, _):
            send1[s, pl.ds(pl.multiple_of(i * SIZE, SIZE), SIZE), :] = product(8 * other + i).astype(BF16)
            return 0

        lax.fori_loop(0, 8, one, 0, unroll=UN)
        send(send1.at[s], s_send.at[s, 0], s1.at[s], partner, recv1.at[s])

    def ours(s):
        def one(i, _):
            part[s, pl.ds(pl.multiple_of(i * SIZE, SIZE), SIZE), :] = product(8 * core + i)
            return 0

        lax.fori_loop(0, 8, one, 0, unroll=UN)

    def chip_sum(s):
        arrived(recv1.at[s], s1.at[s])
        cm = pmass[s] + recv1[s, pl.ds(1024, 16), :].astype(F32)
        mass[s] = cm

        def one(j, _):
            at = pl.ds(pl.multiple_of(j * 256, 256), 256)
            total = part[s, at, :] + recv1[s, at, :].astype(F32)
            chip[s, at, :] = total
            send2[s, j, pl.ds(0, 256), :] = total.astype(BF16)
            send2[s, j, pl.ds(256, 16), :] = cm.astype(BF16)
            return 0

        lax.fori_loop(0, 4, one, 0)
        for k, b in enumerate(PEERS):
            send(send2.at[s, lax.rem(x + b, 4)], s_send.at[s, 1 + k], s2.at[s, k], peers[k], recv2.at[s, k])

    def pair_of(s, xq):
        return state.at[s, pl.ds(pl.multiple_of((8 * core + 2 * xq) * SIZE, 256), 256), :]

    def x_sum(s):
        total = chip[s, pl.ds(pl.multiple_of(x * 256, 256), 256), :]
        m = mass[s]
        for k in range(3):
            arrived(recv2.at[s, k], s2.at[s, k])
            total = total + recv2[s, k, pl.ds(0, 256), :].astype(F32)
            m = m + recv2[s, k, pl.ds(256, 16), :].astype(F32)
        xsum[s] = total
        mass[s] = m
        send3[s, pl.ds(0, 256), :] = total.astype(BF16)
        send3[s, pl.ds(256, 16), :] = m.astype(BF16)
        send(send3.at[s], s_send.at[s, 4], s3.at[s], inner, recv3.at[s])

    def whole_sum(s):
        arrived(recv3.at[s], s3.at[s])
        mass[s] = (mass[s] + recv3[s, pl.ds(256, 16), :].astype(F32)) / count
        mine = pair_of(s, x)
        mine[...] = ((xsum[s] + recv3[s, pl.ds(0, 256), :].astype(F32)) / count).astype(BF16)
        for k in range(3):
            send(mine, s_send.at[s, 5 + k], s4.at[s, k], peers[k])

    def pass_on(s):
        for k, b in enumerate(PEERS):
            arrived(pair_of(s, lax.rem(x + 4 - b, 4)), s4.at[s, k])
        ref = state.at[s, pl.ds(pl.multiple_of(8 * core * SIZE, SIZE), 8 * SIZE), :]
        send(ref, s_send.at[s, 8], s5.at[s], partner)

    def questions(s, part_of):
        if part_of == 0:
            loads[2][s].wait()
            loads[3][s].wait()

        def some(i, _):
            at = pl.ds(pl.multiple_of(16 * i, 16), 16)
            r = to_heads(feature(qb[s, at]).astype(BF16), gb[s, at])
            qh[s, :, at, :] = r[:, :SIZE].astype(BF16).reshape(HEADS, 16, SIZE)
            gate = (count**0.5) / (1.0 + jnp.exp(-r[:, SIZE:]))
            sig[s, :, at, :] = gate.reshape(HEADS, 16, SIZE)
            return 0

        lax.fori_loop(8 * part_of, 8 * part_of + 8, some, 0, unroll=UK)

    def answers(s, side):
        if side is other:
            arrived(state.at[s, pl.ds(pl.multiple_of(8 * other * SIZE, SIZE), 8 * SIZE), :], s5.at[s])

        def one(i, _):
            h = 8 * side + i
            at = pl.ds(pl.multiple_of(h * SIZE, SIZE), SIZE)
            row = mass[s, pl.ds(h, 1), :].astype(BF16)
            right = jnp.concatenate([state[s, at, :], jnp.broadcast_to(row, (SIZE, SIZE))], axis=0)
            r = lax.dot_general(
                qh[s, h, pl.ds(0, ROWS), :], right, (((1,), (1,)), ((), ())), preferred_element_type=F32
            )
            read = r[:, :SIZE] * sig[s, h, pl.ds(0, ROWS), :] / (r[:, SIZE:] + 0.001)
            mixed[pl.ds(s * ROWS, ROWS), at] = read.astype(BF16)
            return 0

        lax.fori_loop(0, 8, one, 0, unroll=UN)

    def project(group, side):
        groups = (0, 1, 2) if group == 2 else (3,)
        for which in range(2):
            if side is other:
                for g in groups:
                    arrived(wbuf[which].at[0, pl.ds(0, 512 if g else 384), :], w_core.at[which, g])
            off, cols = block_cols[which]
            for s in range(SEQS):
                at = pl.ds(s * ROWS, ROWS)
                o = None if group == 2 else acc[which][side, at, :]
                for g in groups:
                    zq = lax.rem((zh, zh + ds, zh - ds, zh + 2)[g] + 4, 4)
                    rows = pl.ds(pl.multiple_of(zq * 512, 512), 512)
                    part_of = jnp.dot(mixed[at, rows], wbuf[which][side, rows, :], preferred_element_type=F32)
                    o = part_of if o is None else o + part_of
                if group == 2:
                    acc[which][side, at, :] = o
                else:
                    out[s, :, pl.ds(pl.multiple_of(1024 * side + off, SIZE), cols)] = o.astype(BF16)

    keys(0, 0)
    questions(1, 0)
    keys(0, 1)
    theirs(0)
    ours(0)
    keys(1, 0)
    chip_sum(0)
    y_got_full(0, 0, 0, 0)
    outer_full(1, 4, 0)
    keys(1, 1)
    theirs(1)
    questions(0, 0)
    y_got_full(0, 0, 0, 1)
    y_got_full(0, 0, 1, 1)
    outer_full(1, 4, 1)
    ours(1)
    chip_sum(1)
    outer_full(0, 0, 1)
    outer_full(0, 0, 0)
    inner_full(1, 4, 0)
    x_sum(0)
    y_got_full(0, 0, 1, 0)
    inner_full(1, 4, 1)
    y_got_half(0, 0, 0)
    outer_full(0, 1, 0)
    y_got_half(0, 0, 1)
    y_got_full(1, 1, 0, 1)
    y_got_full(1, 1, 0, 0)
    y_got_full(1, 1, 1, 1)
    x_sum(1)
    outer_half(1, 4)
    whole_sum(0)
    y_got_full(1, 2, 1, 1)
    questions(1, 1)
    y_got_full(1, 2, 0, 0)
    y_got_full(1, 3, 1, 0)
    y_got_full(1, 2, 1, 0)
    inner_full(0, 1, 0)
    questions(0, 1)
    y_got_full(1, 2, 0, 1)
    inner_full(0, 0, 0)
    y_got_full(1, 3, 1, 1)
    y_got_full(1, 3, 0, 0)
    outer_full(0, 3, 0)
    whole_sum(1)
    outer_full(0, 2, 0)
    y_got_full(1, 3, 0, 1)
    outer_full(0, 3, 1)
    outer_full(0, 2, 1)
    outer_full(0, 1, 1)
    inner_half(1, 4)
    inner_full(0, 3, 0)
    outer_half(0, 1)
    pass_on(0)
    outer_half(0, 0)
    y_got_full(1, 4, 1, 0)
    inner_full(0, 0, 1)
    y_got_half(1, 1, 0)
    inner_full(0, 2, 0)
    answers(0, core)
    inner_full(0, 3, 1)
    y_got_full(1, 1, 1, 0)
    answers(0, other)
    inner_full(0, 2, 1)
    pass_on(1)
    answers(1, core)
    y_got_half(1, 1, 1)
    y_got_half(1, 3, 0)
    y_got_half(1, 2, 1)
    y_got_half(1, 3, 1)
    outer_half(0, 3)
    y_got_full(1, 4, 0, 0)
    y_got_full(1, 4, 1, 1)
    y_got_full(1, 4, 0, 1)
    y_got_half(1, 2, 0)
    inner_full(0, 1, 1)
    answers(1, other)
    outer_half(0, 2)
    project(2, core)
    inner_half(0, 0)
    project(2, other)
    inner_half(0, 1)
    inner_half(0, 3)
    y_got_half(1, 4, 0)
    inner_half(0, 2)
    y_got_half(1, 4, 1)
    project(3, core)
    project(3, other)

    for which in range(2):
        arrived(wbuf[which].at[:, pl.ds(0, 15 * SIZE), :], w_send.at[which])
    for s in range(SEQS):
        arrived(send1.at[s], s_send.at[s, 0])
        for k in range(3):
            arrived(send2.at[s, 0], s_send.at[s, 1 + k])
            arrived(pair_of(s, x), s_send.at[s, 5 + k])
        arrived(send3.at[s], s_send.at[s, 4])
        arrived(state.at[s, pl.ds(0, 8 * SIZE), :], s_send.at[s, 8])


def solution(mesh):
    finer = Mesh(mesh.devices.reshape(4, 4, 2, 4, 2), ("zh", "y", "zl", "x", "core"))
    batch, ctx = ("zh", "y"), ("zl", "x", "core")

    def local(asked_for, offered, contents, gate_rows, out_weight):
        count = float(asked_for.shape[1] * 16)
        dma = pltpu.SemaphoreType.DMA
        vm = pltpu.VMEM
        block = (SEQS, ROWS, HEADS, SIZE)
        return pl.pallas_call(
            lambda *refs: kernel(count, *refs),
            out_shape=jax.ShapeDtypeStruct((SEQS, ROWS, WIDTH), BF16),
            in_specs=[pl.BlockSpec(memory_space=pltpu.HBM)] * 5,
            out_specs=pl.BlockSpec(memory_space=pltpu.VMEM),
            scratch_shapes=[
                vm(block, BF16), vm(block, BF16), vm(block, BF16), vm(block, BF16),
                vm((256, 256), BF16),
                vm((HEADS, ROWS + 16, SIZE), BF16), vm((HEADS, ROWS + 16, SIZE), BF16),
                vm((SEQS, HEADS, ROWS + 16, SIZE), BF16), vm((SEQS, HEADS, ROWS + 8, SIZE), F32),
                vm((SEQS, 1024, SIZE), F32), vm((SEQS, HEADS, SIZE), F32),
                vm((SEQS, 1040, SIZE), BF16), vm((SEQS, 1040, SIZE), BF16),
                vm((SEQS, 1024, SIZE), F32),
                vm((SEQS, 4, 272, SIZE), BF16), vm((SEQS, 3, 272, SIZE), BF16),
                vm((SEQS, 256, SIZE), F32), vm((SEQS, HEADS, SIZE), F32),
                vm((SEQS, 272, SIZE), BF16), vm((SEQS, 272, SIZE), BF16),
                vm((SEQS, WIDTH, SIZE), BF16),
                vm((SEQS * ROWS, WIDTH), BF16),
                vm((2, WIDTH, CUT), BF16), vm((2, WIDTH, 1024 - CUT), BF16),
                vm((2, SEQS * ROWS, CUT), F32), vm((2, SEQS * ROWS, 1024 - CUT), F32),
                dma((12,)),
                dma((2, 2, 5, 2)), dma((2, 2, 5, 2)),
                dma((2,)), dma((2, 4)), dma((SEQS, 9)),
                dma((SEQS,)), dma((SEQS, 3)), dma((SEQS,)), dma((SEQS, 3)), dma((SEQS,)),
            ],
            compiler_params=pltpu.CompilerParams(
                collective_id=0, has_side_effects=True, vmem_limit_bytes=48 * 1024 * 1024
            ),
        )(*(pltpu.with_memory_space_constraint(a, pltpu.HBM) for a in (asked_for, offered, contents, gate_rows, out_weight)))

    cut = P(batch, ctx, None, None)
    return jax.shard_map(
        local, mesh=finer, in_specs=(cut, cut, cut, cut, P(batch, None)), out_specs=P(batch, ctx, None), check_vma=False
    )
```

```python
import jax
import jax.numpy as jnp
from jax import lax
from jax.experimental import pallas as pl
from jax.experimental.pallas import tpu as pltpu
from jax.sharding import Mesh
from jax.sharding import PartitionSpec as P

F32, BF16 = jnp.float32, jnp.bfloat16
MESH = pl.DeviceIdType.MESH
HEADS, SIZE = 16, 128
SEQS, ROWS = 2, 256
WIDTH = HEADS * SIZE
HALF = SIZE // 2
CUT = 384
UN, UK = 8, 4
OFFSETS = (0, 3, 1, 2, 0)
PEERS = (2, 1, 3)


def feature(x):
    wide = x.astype(F32)
    return jnp.where(wide > 0.0, wide + 1.0, jnp.exp(jnp.minimum(wide, 0.0)))


def kernel(
    count, q_hbm, k_hbm, v_hbm, g_hbm, w_hbm, out,
    qb, kb, vb, gb, perm, kh, vh, qh, sig, part, pmass, send1, recv1, chip, send2, recv2, xsum, mass,
    send3, recv3, state, mixed, wa, wb, acca, accb,
    ld, ya, za, w_send, w_core, s_send, s1, s2, s3, s4, s5,
):
    zh, y, zl, x, core = (lax.axis_index(a) for a in ("zh", "y", "zl", "x", "core"))
    other = 1 - core
    z = 2 * zh + zl
    ds = 2 * zl - 1
    zo, zi = lax.rem(z + ds + 8, 8), lax.rem(z - ds + 8, 8)
    outer = {"zh": zo // 2, "zl": lax.rem(zo, 2)}
    inner = {"zh": zi // 2, "zl": lax.rem(zi, 2)}
    ynext = [{"y": lax.rem(y + 1, 4)}, {"y": lax.rem(y + 3, 4)}]
    peers = [{"x": lax.rem(x + b, 4)} for b in PEERS]
    partner = {"core": other}

    own = (zh * 4 + y) * SIZE
    wbuf, acc = (wa, wb), (acca, accb)
    block_cols = ((0, CUT), (CUT, 1024 - CUT))
    wloads = [
        pltpu.make_async_copy(
            w_hbm.at[:, pl.ds(1024 * c + block_cols[which][0], block_cols[which][1])],
            wbuf[which].at[c, pl.ds(pl.multiple_of(own, SIZE), SIZE), :],
            ld.at[2 * c + which],
        )
        for which in range(2)
        for c in range(2)
    ]
    loads = [
        [pltpu.make_async_copy(h.at[s], b.at[s], ld.at[4 + 2 * i + s]) for s in range(SEQS)]
        for i, (h, b) in enumerate(((k_hbm, kb), (v_hbm, vb), (q_hbm, qb), (g_hbm, gb)))
    ]
    for c in wloads:
        c.start()
    for s in range(SEQS):
        loads[0][s].start()
        loads[1][s].start()
    for s in range(SEQS):
        loads[2][s].start()
        loads[3][s].start()

    barrier = pltpu.get_barrier_semaphore()
    for dev in (partner, outer, inner, *ynext, *peers):
        pl.semaphore_signal(barrier, inc=1, device_id=dev, device_id_type=MESH)
    row = lax.broadcasted_iota(jnp.int32, (256, 256), 0)
    col = lax.broadcasted_iota(jnp.int32, (256, 256), 1)
    perm[...] = jnp.where(col == (row & 15) * 16 + (row >> 4), 1.0, 0.0).astype(BF16)
    pl.semaphore_wait(barrier, 8)

    def send(src, ssem, rsem, dev, dst=None):
        pltpu.make_async_remote_copy(
            src_ref=src, dst_ref=src if dst is None else dst, send_sem=ssem, recv_sem=rsem,
            device_id=dev, device_id_type=MESH,
        ).start()

    def arrived(ref, rsem):
        pltpu.make_async_copy(ref, ref, rsem).wait()

    def piece(which, zq, yq, u):
        at = (lax.rem(zq + 8, 4) * 4 + lax.rem(yq + 8, 4)) * SIZE + u * HALF
        return wbuf[which].at[core, pl.ds(pl.multiple_of(at, HALF), HALF), :]

    def share(ref, which, group):
        send(ref, w_send.at[which], w_core.at[which, group], partner)

    y_zq = (zh, zh, zh + ds, zh - ds, zh + 2)
    y_half = ((0, 1), (0, 1), (zl, 1 - zl), (1 - zl, zl), (zl, 1 - zl))

    def y_send(which, slot, d, u):
        send(piece(which, y_zq[slot], y, u), w_send.at[which], ya.at[d, 0, slot, u], ynext[d])

    def y_got_full(which, slot, d, f):
        u = y_half[slot][f]
        ref = piece(which, y_zq[slot], y - (1 - 2 * d), u)
        arrived(ref, ya.at[d, 0, slot, u])

        def onward():
            send(ref, w_send.at[which], ya.at[d, 1, slot, 0], ynext[d])

        if slot < 2:
            if u == d:
                onward()
        else:
            pl.when(u == d)(onward)
        share(ref, which, (0, 0, 1, 2, 3)[slot])
        if which == 0:
            z_own(0, 1 + d, u)

    def y_got_half(which, slot, d):
        ref = piece(which, y_zq[slot], y + 2, d)
        arrived(ref, ya.at[d, 1, slot, 0])
        share(ref, which, (0, 0, 1, 2, 3)[slot])
        if which == 0:
            z_own(0, 3, d)

    def z_own(which, slot, u):
        send(piece(which, zh, y + OFFSETS[slot], u), w_send.at[which], za.at[0, 0, slot, u], outer)

    def to_y(which, slot, u):
        if which == 1:
            for d in range(2):
                y_send(1, slot, d, u)

    def outer_full(which, slot, f):
        u = (zl, 1 - zl)[f]
        ref = piece(which, zh + ds, y + OFFSETS[slot], u)
        arrived(ref, za.at[0, 0, slot, u])
        send(ref, w_send.at[which], za.at[1, 0, slot, u], inner)
        to_y(which, 2, u)
        share(ref, which, 1)

    def inner_full(which, slot, f):
        u = (1 - zl, zl)[f]
        ref = piece(which, zh - ds, y + OFFSETS[slot], u)
        arrived(ref, za.at[1, 0, slot, u])
        if f == 0:
            send(ref, w_send.at[which], za.at[0, 1, slot, 0], outer)
        to_y(which, 3, u)
        share(ref, which, 2)

    def outer_half(which, slot):
        ref = piece(which, zh + 2, y + OFFSETS[slot], zl)
        arrived(ref, za.at[0, 1, slot, 0])
        send(ref, w_send.at[which], za.at[1, 1, slot, 0], inner)
        to_y(which, 4, zl)
        share(ref, which, 3)

    def inner_half(which, slot):
        ref = piece(which, zh + 2, y + OFFSETS[slot], 1 - zl)
        arrived(ref, za.at[1, 1, slot, 0])
        to_y(which, 4, 1 - zl)
        share(ref, which, 3)

    for c in wloads:
        c.wait()
    for f in range(2):
        for d in range(2):
            y_send(0, 0, d, (d, 1 - d)[f])
        z_own(1, 4, (1 - zl, zl)[f])
    for f in range(2):
        z_own(0, 0, (1 - zl, zl)[f])
        for d in range(2):
            y_send(1, 1, d, (d, 1 - d)[f])

    def to_heads(left, right):
        both = jnp.concatenate([left.reshape(256, SIZE), right.reshape(256, SIZE)], axis=1)
        return jnp.dot(perm[...], both, preferred_element_type=F32)

    def keys(s, part_of):
        if part_of == 0:
            loads[0][s].wait()
            loads[1][s].wait()

        def some(i, total):
            at = pl.ds(pl.multiple_of(16 * i, 16), 16)
            kf = feature(kb[s, at]).astype(BF16)
            r = to_heads(kf, vb[s, at])
            kh[:, at, :] = r[:, :SIZE].astype(BF16).reshape(HEADS, 16, SIZE)
            vh[:, at, :] = r[:, SIZE:].astype(BF16).reshape(HEADS, 16, SIZE)
            return total + jnp.sum(kf.astype(F32), axis=0)

        start = jnp.zeros((HEADS, SIZE), F32) if part_of == 0 else pmass[s]
        total = lax.fori_loop(8 * part_of, 8 * part_of + 8, some, start, unroll=UK)
        pmass[s] = total
        if part_of == 1:
            send1[s, pl.ds(1024, 16), :] = total.astype(BF16)

    def product(h):
        return lax.dot_general(
            vh[h, pl.ds(0, ROWS), :], kh[h, pl.ds(0, ROWS), :], (((0,), (0,)), ((), ())), preferred_element_type=F32
        )

    def theirs(s):
        def one(i, _):
            send1[s, pl.ds(pl.multiple_of(i * SIZE, SIZE), SIZE), :] = product(8 * other + i).astype(BF16)
            return 0

        lax.fori_loop(0, 8, one, 0, unroll=UN)
        send(send1.at[s], s_send.at[s, 0], s1.at[s], partner, recv1.at[s])

    def ours(s):
        def one(i, _):
            part[s, pl.ds(pl.multiple_of(i * SIZE, SIZE), SIZE), :] = product(8 * core + i)
            return 0

        lax.fori_loop(0, 8, one, 0, unroll=UN)

    def chip_sum(s):
        arrived(recv1.at[s], s1.at[s])
        cm = pmass[s] + recv1[s, pl.ds(1024, 16), :].astype(F32)
        mass[s] = cm

        def one(j, _):
            at = pl.ds(pl.multiple_of(j * 256, 256), 256)
            total = part[s, at, :] + recv1[s, at, :].astype(F32)
            chip[s, at, :] = total
            send2[s, j, pl.ds(0, 256), :] = total.astype(BF16)
            send2[s, j, pl.ds(256, 16), :] = cm.astype(BF16)
            return 0

        lax.fori_loop(0, 4, one, 0)
        for k, b in enumerate(PEERS):
            send(send2.at[s, lax.rem(x + b, 4)], s_send.at[s, 1 + k], s2.at[s, k], peers[k], recv2.at[s, k])

    def pair_of(s, xq):
        return state.at[s, pl.ds(pl.multiple_of((8 * core + 2 * xq) * SIZE, 256), 256), :]

    def x_sum(s):
        total = chip[s, pl.ds(pl.multiple_of(x * 256, 256), 256), :]
        m = mass[s]
        for k in range(3):
            arrived(recv2.at[s, k], s2.at[s, k])
            total = total + recv2[s, k, pl.ds(0, 256), :].astype(F32)
            m = m + recv2[s, k, pl.ds(256, 16), :].astype(F32)
        xsum[s] = total
        mass[s] = m
        send3[s, pl.ds(0, 256), :] = total.astype(BF16)
        send3[s, pl.ds(256, 16), :] = m.astype(BF16)
        send(send3.at[s], s_send.at[s, 4], s3.at[s], inner, recv3.at[s])

    def whole_sum(s):
        arrived(recv3.at[s], s3.at[s])
        mass[s] = (mass[s] + recv3[s, pl.ds(256, 16), :].astype(F32)) / count
        mine = pair_of(s, x)
        mine[...] = ((xsum[s] + recv3[s, pl.ds(0, 256), :].astype(F32)) / count).astype(BF16)
        for k in range(3):
            send(mine, s_send.at[s, 5 + k], s4.at[s, k], peers[k])

    def pass_on(s):
        for k, b in enumerate(PEERS):
            arrived(pair_of(s, lax.rem(x + 4 - b, 4)), s4.at[s, k])
        ref = state.at[s, pl.ds(pl.multiple_of(8 * core * SIZE, SIZE), 8 * SIZE), :]
        send(ref, s_send.at[s, 8], s5.at[s], partner)

    def questions(s, part_of):
        if part_of == 0:
            loads[2][s].wait()
            loads[3][s].wait()

        def some(i, _):
            at = pl.ds(pl.multiple_of(16 * i, 16), 16)
            r = to_heads(feature(qb[s, at]).astype(BF16), gb[s, at])
            qh[s, :, at, :] = r[:, :SIZE].astype(BF16).reshape(HEADS, 16, SIZE)
            gate = (count**0.5) / (1.0 + jnp.exp(-r[:, SIZE:]))
            sig[s, :, at, :] = gate.reshape(HEADS, 16, SIZE)
            return 0

        lax.fori_loop(8 * part_of, 8 * part_of + 8, some, 0, unroll=UK)

    def answers(s, side):
        if side is other:
            arrived(state.at[s, pl.ds(pl.multiple_of(8 * other * SIZE, SIZE), 8 * SIZE), :], s5.at[s])

        def one(i, _):
            h = 8 * side + i
            at = pl.ds(pl.multiple_of(h * SIZE, SIZE), SIZE)
            row = mass[s, pl.ds(h, 1), :].astype(BF16)
            right = jnp.concatenate([state[s, at, :], jnp.broadcast_to(row, (SIZE, SIZE))], axis=0)
            r = lax.dot_general(
                qh[s, h, pl.ds(0, ROWS), :], right, (((1,), (1,)), ((), ())), preferred_element_type=F32
            )
            read = r[:, :SIZE] * sig[s, h, pl.ds(0, ROWS), :] / (r[:, SIZE:] + 0.001)
            mixed[pl.ds(s * ROWS, ROWS), at] = read.astype(BF16)
            return 0

        lax.fori_loop(0, 8, one, 0, unroll=UN)

    def project(group, side):
        groups = (0, 1, 2) if group == 2 else (3,)
        for which in range(2):
            if side is other:
                for g in groups:
                    arrived(wbuf[which].at[0, pl.ds(0, 512 if g else 384), :], w_core.at[which, g])
            off, cols = block_cols[which]
            for s in range(SEQS):
                at = pl.ds(s * ROWS, ROWS)
                o = None if group == 2 else acc[which][side, at, :]
                for g in groups:
                    zq = lax.rem((zh, zh + ds, zh - ds, zh + 2)[g] + 4, 4)
                    rows = pl.ds(pl.multiple_of(zq * 512, 512), 512)
                    part_of = jnp.dot(mixed[at, rows], wbuf[which][side, rows, :], preferred_element_type=F32)
                    o = part_of if o is None else o + part_of
                if group == 2:
                    acc[which][side, at, :] = o
                else:
                    out[s, :, pl.ds(pl.multiple_of(1024 * side + off, SIZE), cols)] = o.astype(BF16)

    keys(0, 0)
    keys(0, 1)
    theirs(0)
    ours(0)
    keys(1, 0)
    chip_sum(0)
    keys(1, 1)
    theirs(1)
    outer_full(1, 4, 0)
    ours(1)
    y_got_full(0, 0, 0, 0)
    questions(0, 0)
    chip_sum(1)
    y_got_full(0, 0, 1, 1)
    outer_full(1, 4, 1)
    y_got_full(1, 1, 0, 0)
    y_got_full(0, 0, 0, 1)
    outer_full(0, 0, 0)
    questions(0, 1)
    outer_full(0, 0, 1)
    y_got_full(1, 1, 1, 1)
    inner_full(1, 4, 0)
    y_got_full(0, 0, 1, 0)
    x_sum(0)
    outer_full(0, 1, 0)
    y_got_full(1, 1, 0, 1)
    y_got_full(1, 2, 0, 0)
    y_got_half(0, 0, 0)
    questions(1, 0)
    x_sum(1)
    y_got_half(0, 0, 1)
    inner_full(0, 0, 1)
    inner_full(1, 4, 1)
    outer_half(1, 4)
    whole_sum(0)
    inner_full(0, 0, 0)
    inner_full(0, 1, 0)
    outer_full(0, 2, 0)
    y_got_full(1, 2, 0, 1)
    y_got_full(1, 3, 1, 0)
    y_got_full(1, 2, 1, 1)
    y_got_full(1, 2, 1, 0)
    outer_full(0, 3, 0)
    outer_full(0, 2, 1)
    whole_sum(1)
    inner_half(1, 4)
    y_got_half(1, 1, 1)
    outer_full(0, 1, 1)
    inner_full(0, 2, 0)
    outer_full(0, 3, 1)
    y_got_full(1, 3, 0, 0)
    y_got_full(1, 3, 0, 1)
    questions(1, 1)
    outer_half(0, 0)
    pass_on(0)
    outer_half(0, 1)
    inner_full(0, 3, 0)
    y_got_full(1, 3, 1, 1)
    y_got_full(1, 4, 0, 0)
    y_got_half(1, 2, 0)
    y_got_half(1, 1, 0)
    answers(0, other)
    pass_on(1)
    y_got_full(1, 4, 1, 0)
    y_got_full(1, 4, 0, 1)
    outer_half(0, 2)
    y_got_full(1, 4, 1, 1)
    answers(1, core)
    inner_full(0, 1, 1)
    answers(0, core)
    inner_full(0, 3, 1)
    inner_full(0, 2, 1)
    answers(1, other)
    inner_half(0, 0)
    y_got_full(1, 1, 1, 0)
    outer_half(0, 3)
    y_got_half(1, 2, 1)
    y_got_half(1, 3, 0)
    y_got_half(1, 3, 1)
    project(2, core)
    inner_half(0, 2)
    inner_half(0, 1)
    project(2, other)
    y_got_half(1, 4, 0)
    y_got_half(1, 4, 1)
    inner_half(0, 3)
    project(3, core)
    project(3, other)

    for which in range(2):
        arrived(wbuf[which].at[:, pl.ds(0, 15 * SIZE), :], w_send.at[which])
    for s in range(SEQS):
        arrived(send1.at[s], s_send.at[s, 0])
        for k in range(3):
            arrived(send2.at[s, 0], s_send.at[s, 1 + k])
            arrived(pair_of(s, x), s_send.at[s, 5 + k])
        arrived(send3.at[s], s_send.at[s, 4])
        arrived(state.at[s, pl.ds(0, 8 * SIZE), :], s_send.at[s, 8])


def solution(mesh):
    finer = Mesh(mesh.devices.reshape(4, 4, 2, 4, 2), ("zh", "y", "zl", "x", "core"))
    batch, ctx = ("zh", "y"), ("zl", "x", "core")

    def local(asked_for, offered, contents, gate_rows, out_weight):
        count = float(asked_for.shape[1] * 16)
        dma = pltpu.SemaphoreType.DMA
        vm = pltpu.VMEM
        block = (SEQS, ROWS, HEADS, SIZE)
        return pl.pallas_call(
            lambda *refs: kernel(count, *refs),
            out_shape=jax.ShapeDtypeStruct((SEQS, ROWS, WIDTH), BF16),
            in_specs=[pl.BlockSpec(memory_space=pltpu.HBM)] * 5,
            out_specs=pl.BlockSpec(memory_space=pltpu.VMEM),
            scratch_shapes=[
                vm(block, BF16), vm(block, BF16), vm(block, BF16), vm(block, BF16),
                vm((256, 256), BF16),
                vm((HEADS, ROWS + 16, SIZE), BF16), vm((HEADS, ROWS + 16, SIZE), BF16),
                vm((SEQS, HEADS, ROWS + 16, SIZE), BF16), vm((SEQS, HEADS, ROWS + 8, SIZE), F32),
                vm((SEQS, 1024, SIZE), F32), vm((SEQS, HEADS, SIZE), F32),
                vm((SEQS, 1040, SIZE), BF16), vm((SEQS, 1040, SIZE), BF16),
                vm((SEQS, 1024, SIZE), F32),
                vm((SEQS, 4, 272, SIZE), BF16), vm((SEQS, 3, 272, SIZE), BF16),
                vm((SEQS, 256, SIZE), F32), vm((SEQS, HEADS, SIZE), F32),
                vm((SEQS, 272, SIZE), BF16), vm((SEQS, 272, SIZE), BF16),
                vm((SEQS, WIDTH, SIZE), BF16),
                vm((SEQS * ROWS, WIDTH), BF16),
                vm((2, WIDTH, CUT), BF16), vm((2, WIDTH, 1024 - CUT), BF16),
                vm((2, SEQS * ROWS, CUT), F32), vm((2, SEQS * ROWS, 1024 - CUT), F32),
                dma((12,)),
                dma((2, 2, 5, 2)), dma((2, 2, 5, 2)),
                dma((2,)), dma((2, 4)), dma((SEQS, 9)),
                dma((SEQS,)), dma((SEQS, 3)), dma((SEQS,)), dma((SEQS, 3)), dma((SEQS,)),
            ],
            compiler_params=pltpu.CompilerParams(
                collective_id=0, has_side_effects=True, vmem_limit_bytes=48 * 1024 * 1024
            ),
        )(*(pltpu.with_memory_space_constraint(a, pltpu.HBM) for a in (asked_for, offered, contents, gate_rows, out_weight)))

    cut = P(batch, ctx, None, None)
    return jax.shard_map(
        local, mesh=finer, in_specs=(cut, cut, cut, cut, P(batch, None)), out_specs=P(batch, ctx, None), check_vma=False
    )
```
